32 devices in a mesh: groups: 2 (over y), pages: 4 (over z), heads: 4 (over x, core).
Axes of the slice: x: 2, y: 2, z: 4, core: 2. Of those that a mesh axis runs over, the one named last changes fastest.
Arguments:
- q_nope: bfloat16 [256, 16384], P(('groups', 'pages'), 'heads'), parts along dimension 0, may hold values from -6 to 6
- q_rope: bfloat16 [256, 8192], P(('groups', 'pages'), 'heads'), parts along dimension 0, may hold values from -16 to 16
- cache_tiles: bfloat16 [12288, 576], P(('groups', 'pages')), parts along dimension 0, may hold values from -8 to 8
- absorb_keys: bfloat16 [128, 128, 512], P('heads'), may hold values from -0.5 to 0.5
- absorb_values: bfloat16 [128, 512, 128], P('heads'), may hold values from -2 to 2
- page_counts: int32 [8], P('groups'), parts along dimension 0, may hold values from 1 to 24, as said below
- query_token: int32 [256], P('groups'), parts along dimension 0, may hold values from 0 to 127, each once
- query_offsets: int32 [256], P('groups'), parts along dimension 0, may hold values from 512 to 2048
Outputs:
- attention_out: bfloat16 [256, 16384], P(('groups', 'pages'), 'heads'), parts along dimension 0
The draws below stay inside these ranges and needn't reach their ends.
There are 2 independent parts, one for each index of `groups`. The reference program is written for one: setup_inputs(seed, part) draws one part's arguments, and reference() takes and returns one part's arrays. A program takes and returns all parts, laid end to end along the dimension named above; an argument that names none is the same for every part. Nothing has to cross between parts.
Inputs may be any that keep to these rules, and one draw needn't show every extreme that they name: Member m's live pages are its first page_counts[m] page slots; the counts sum to 32. `query_token`: a permutation of the span's tokens. Token t attends to the live cache rows whose key_position is below query_offsets[t].
All inputs are finite; a program needn't handle non-finite values.
Results may differ from the reference program's by a relative error of at most 0.022.
Values may be sent and summed in bfloat16 or wider, within the bound.
No kernel may reach another device: no remote copies, remote signals or barrier semaphores. Data moves between devices by JAX's collectives and lax.ppermute only.
A program may use at most 64 MiB of HBM per device.

```python
import jax
import jax.numpy as jnp
from jax import lax

HEADS = 128
NOPE = 128
ROPE = 64
LATENT = 512
VHEAD = 128
PAGE = 64
QUERIES = 128
MEMBERS = 4
CAP = 24
TOTAL_PAGES = 32
CACHE_ROWS = 6144


def draw_page_counts(key, part):
    shuffled = jax.random.permutation(jax.random.fold_in(key, 91), MEMBERS).astype(jnp.int32)
    ranks = jnp.zeros((MEMBERS,), jnp.int32).at[shuffled].set(jnp.arange(MEMBERS, dtype=jnp.int32))
    heavy_count = max(MEMBERS // 4, 1)
    light_count = MEMBERS - heavy_count
    leftover = TOTAL_PAGES - heavy_count * CAP
    spare = leftover - light_count
    grid_slots = light_count * (CAP - 1)
    placed = jax.random.permutation(jax.random.fold_in(key, 97), grid_slots).astype(jnp.int32)
    chosen = (placed < spare).astype(jnp.int32).reshape(light_count, CAP - 1)
    light_counts = 1 + jnp.sum(chosen, axis=1).astype(jnp.int32)
    light_rank = jnp.clip(ranks - heavy_count, 0, light_count - 1)
    light_value = light_counts[light_rank]
    return jnp.where(ranks < heavy_count, jnp.int32(CAP), light_value).astype(jnp.int32)


def draw_cache_tiles(key, part):
    first = jax.random.fold_in(jax.random.fold_in(key, 31), 0)
    tiles = jnp.clip(jax.random.normal(first, (CACHE_ROWS, LATENT + ROPE), jnp.float32), -6.0, 6.0)
    return tiles.astype(jnp.bfloat16)


def draw_q_rope(key, part):
    first = jax.random.fold_in(key, 53)
    values = jnp.clip(jax.random.normal(first, (QUERIES, HEADS, ROPE), jnp.float32), -6.0, 6.0)
    return values.reshape(QUERIES, HEADS * ROPE).astype(jnp.bfloat16)


def touch_ends(entries, stream_key, smallest, high):
    longest = entries.shape.index(max(entries.shape))
    spots = []
    for shift in (0, 1):
        where = [jax.random.randint(jax.random.fold_in(stream_key, axis), (), 0, length) for axis, length in enumerate(entries.shape)]
        where[longest] = (where[longest] + shift) % entries.shape[longest]
        spots.append(tuple(where))
    return entries.at[spots[0]].set(smallest).at[spots[1]].set(high)


def block_levels(stream_key, shape, pieces, least, high):
    gain = 1.0
    for dim, parts in pieces:
        draws = jax.random.uniform(jax.random.fold_in(jax.random.fold_in(stream_key, 6), dim), (parts,), jnp.float32, least / len(pieces), high / len(pieces))
        gain = gain * jnp.repeat(jnp.exp(draws), shape[dim] // parts).reshape((-1,) + (1,) * (len(shape) - 1 - dim))
    return gain


def normal_values(key, extent, spread, most, pieces=(), held_as=jnp.bfloat16):
    entries = jax.random.normal(key, extent, jnp.float32) * spread
    if len(pieces) > 0:
        entries = block_levels(key, extent, pieces, -0.22, 0.18) * entries
    return jnp.clip(entries, min=-most, max=most).astype(held_as)


def setup_inputs(seed: int = 0, part: int = 0) -> dict:
    key_list = jax.random.split(jax.random.key(seed), 9)
    own_keys = jax.random.split(jax.random.fold_in(key_list[8], part), 9)
    return {
        "q_nope": normal_values(own_keys[0], (QUERIES, HEADS * NOPE), 1.0, 6.0, ((0, 4), (1, 4))),
        "q_rope": draw_q_rope(jax.random.fold_in(jax.random.fold_in(key_list[8], part), 71), part),
        "cache_tiles": draw_cache_tiles(jax.random.fold_in(jax.random.fold_in(key_list[8], part), 71), part),
        "absorb_keys": normal_values(key_list[3], (HEADS, NOPE, LATENT), NOPE ** -0.5, 0.5, ((0, 4),)),
        "absorb_values": normal_values(key_list[4], (HEADS, LATENT, VHEAD), 8 ** -0.5, 2.0, ((0, 4),)),
        "page_counts": draw_page_counts(jax.random.fold_in(jax.random.fold_in(key_list[8], part), 71), part),
        "query_token": jax.random.permutation(own_keys[6], QUERIES).astype(jnp.int32),
        "query_offsets": touch_ends(jax.random.randint(own_keys[7], (QUERIES,), PAGE * TOTAL_PAGES // 4, PAGE * TOTAL_PAGES + 1), jax.random.fold_in(own_keys[7], 1), PAGE * TOTAL_PAGES // 4, PAGE * TOTAL_PAGES).astype(jnp.int32),
    }


def reference(q_nope, q_rope, cache_tiles, absorb_keys, absorb_values, page_counts, query_token, query_offsets):
    slot_pages = CAP
    prefix = jnp.cumsum(page_counts) - page_counts
    slots = jnp.arange(MEMBERS * slot_pages, dtype=jnp.int32)
    member = slots // slot_pages
    within = slots % slot_pages
    live = within < page_counts[member]
    logical = prefix[member] + within
    inside = jnp.arange(PAGE, dtype=jnp.int32)
    positions = logical[:, None] * PAGE + inside[None, :]
    positions = jnp.where(live[:, None], positions, jnp.int32(2 ** 30)).reshape(-1)
    inverse = jnp.zeros((QUERIES,), jnp.int32).at[query_token].set(jnp.arange(QUERIES, dtype=jnp.int32))
    visible = positions[None, :] < query_offsets[:, None]
    group_heads = 8
    group_count = HEADS // group_heads
    nope_tok = q_nope[inverse].reshape(QUERIES, group_count, group_heads, NOPE).transpose(1, 0, 2, 3)
    rope_tok = q_rope[inverse].reshape(QUERIES, group_count, group_heads, ROPE).transpose(1, 0, 2, 3)
    keys_grouped = absorb_keys.reshape(group_count, group_heads, NOPE, LATENT)
    values_grouped = absorb_values.reshape(group_count, group_heads, LATENT, VHEAD)
    scale = (NOPE + ROPE) ** -0.5
    latent_part = cache_tiles[:, :LATENT]

    def one_group(inputs):
        nope_part, rope_part, keys_part, values_part = inputs
        q_latent = jnp.einsum("qhn,hnl->qhl", nope_part.astype(jnp.float32), keys_part.astype(jnp.float32),
                              precision=lax.Precision.HIGHEST).astype(jnp.bfloat16)
        full = jnp.concatenate([q_latent, rope_part], axis=-1).reshape(QUERIES * group_heads, LATENT + ROPE)
        scores = jnp.dot(full, cache_tiles.T, preferred_element_type=jnp.float32)
        scores = scores.reshape(QUERIES, group_heads, -1) * scale
        mask = visible[:, None, :]
        row_max = jnp.max(jnp.where(mask, scores, -jnp.inf), axis=-1, keepdims=True)
        weights = jnp.where(mask, jnp.exp(scores - row_max), 0.0)
        denominator = jnp.sum(weights, axis=-1)
        rounded = weights.astype(jnp.bfloat16).reshape(QUERIES * group_heads, -1)
        summed = jnp.dot(rounded, latent_part, preferred_element_type=jnp.float32).reshape(QUERIES, group_heads, LATENT)
        latent_out = summed / denominator[..., None]
        return jnp.einsum("qhl,hlv->qhv", latent_out, values_part.astype(jnp.float32),
                          precision=lax.Precision.HIGHEST)

    outputs = lax.map(one_group, (nope_tok, rope_tok, keys_grouped, values_grouped))
    return outputs.transpose(1, 0, 2, 3).reshape(QUERIES, HEADS * VHEAD).astype(jnp.bfloat16)
```

```python
import functools

import jax
import jax.numpy as jnp
from jax import lax
from jax.experimental import pallas as pl
from jax.experimental.pallas import tpu as pltpu
from jax.sharding import PartitionSpec as P

PAGE = 64
GROUP = 2
LANES = 4
BLOCK_PAGES = 8
HEADS_STEP = 4

FLOOR = -1e30
FAR = 2**30
LOG2E = 1.4426950408889634


def attend_kernel(
    dims,
    scal_ref,
    q_ref,
    tok_ref,
    lim_ref,
    own_ref,
    part0_ref,
    part1_ref,
    part2_ref,
    part3_ref,
    keys_ref,
    values_ref,
    out_ref,
    qs,
    mx,
    den,
    acc,
    lse,
):
    hh, hb, nope, rope, latent, vhead, rows = dims
    step = pl.program_id(0)
    steps = hh // hb
    block = BLOCK_PAGES * PAGE
    scale2 = (nope + rope) ** (-0.5) * LOG2E
    nt = (((1,), (1,)), ((), ()))

    @pl.when(step == 0)
    def _():
        lse[...] = jnp.zeros_like(lse)

    for h in range(hb):
        lat = jnp.dot(q_ref[:, pl.ds(pl.multiple_of((step * hb + h) * nope, nope), nope)], keys_ref[h],
                      preferred_element_type=jnp.float32)
        qs[h * rows:(h + 1) * rows, :latent] = lat.astype(jnp.bfloat16)
    for pair in range(hb // 2):
        both = q_ref[:, pl.ds(pl.multiple_of(hh * nope + (step * hb // 2 + pair) * 2 * rope, 2 * rope), 2 * rope)]
        for e in range(2):
            h = 2 * pair + e
            qs[h * rows:(h + 1) * rows, latent:] = both[:, e * rope:(e + 1) * rope]

    mx[...] = jnp.full_like(mx, FLOOR)
    den[...] = jnp.zeros_like(den)
    acc[...] = jnp.zeros_like(acc)
    limit = jnp.concatenate([lim_ref[...]] * hb, axis=0)

    def attend(tiles, positions):
        scores = lax.dot_general(qs[...], tiles, nt, preferred_element_type=jnp.float32)
        mask = positions < limit
        scores = jnp.where(mask, scores, FLOOR)
        old = mx[...]
        new = jnp.maximum(old, jnp.max(scores, axis=1, keepdims=True))
        weights = jnp.where(mask, jnp.exp2((scores - new) * scale2), 0.0)
        keep = jnp.exp2((old - new) * scale2)
        mx[...] = new
        den[...] = den[...] * keep + jnp.sum(weights, axis=1, keepdims=True)
        acc[...] = acc[...] * keep + jnp.dot(
            weights.astype(jnp.bfloat16), tiles[:, :latent], preferred_element_type=jnp.float32
        )

    lane = lax.broadcasted_iota(jnp.int32, (1, block), 1)

    def own_block(j, _):
        live = scal_ref[0]
        tiles = own_ref[pl.ds(pl.multiple_of(j * block, block), block), :]
        page = j * BLOCK_PAGES + lane // PAGE
        positions = scal_ref[1] * PAGE + j * block + lane
        attend(tiles, jnp.where(page < live, positions, FAR))
        return 0

    lax.fori_loop(0, (scal_ref[0] + BLOCK_PAGES - 1) // BLOCK_PAGES, own_block, 0)

    sub = PAGE // LANES
    width = BLOCK_PAGES * sub

    def partner_block(j, _):
        live = scal_ref[2]
        refs = (part0_ref, part1_ref, part2_ref, part3_ref)
        tiles = jnp.concatenate([r[pl.ds(pl.multiple_of(j * width, width), width), :] for r in refs], axis=0)
        piece, inner = lane // width, lane % width
        quarter = jnp.where(piece == 0, scal_ref[5], jnp.where(piece == 1, scal_ref[6],
                            jnp.where(piece == 2, scal_ref[7], scal_ref[8])))
        page = j * BLOCK_PAGES + inner // sub
        positions = (scal_ref[3] + page) * PAGE + quarter * sub + inner % sub
        attend(tiles, jnp.where(page < live, positions, FAR))
        return 0

    lax.fori_loop(0, (scal_ref[2] + BLOCK_PAGES - 1) // BLOCK_PAGES, partner_block, 0)

    order = (tok_ref[...] == lax.broadcasted_iota(jnp.int32, (rows, rows), 0)).astype(jnp.bfloat16)
    total = den[...]
    seen = total > 0.0
    latent_out = (acc[...] * jnp.where(seen, 1.0 / jnp.where(seen, total, 1.0), 0.0)).astype(jnp.bfloat16)
    logs = jnp.where(seen, mx[...] * scale2 + jnp.log2(jnp.where(seen, total, 1.0)), FLOOR)
    column = lax.broadcasted_iota(jnp.int32, (rows, 128), 1)
    for h in range(hb):
        part = slice(h * rows, (h + 1) * rows)
        value = jnp.dot(latent_out[part], values_ref[h], preferred_element_type=jnp.float32).astype(jnp.bfloat16)
        value = jnp.dot(order, value, preferred_element_type=jnp.float32).astype(jnp.bfloat16)
        out_ref[:, pl.ds(pl.multiple_of((step * hb + h) * vhead, vhead), vhead)] = value
        full = logs[part]
        high = full.astype(jnp.bfloat16).astype(jnp.float32)
        middle = (full - high).astype(jnp.bfloat16).astype(jnp.float32)
        low = full - high - middle
        head = step * hb + h
        lse[...] = jnp.where(column == head, high, jnp.where(column == hh + head, middle,
                             jnp.where(column == 2 * hh + head, low, lse[...])))

    @pl.when(step == steps - 1)
    def _():
        ordered = jnp.dot(order, lse[...].astype(jnp.bfloat16), preferred_element_type=jnp.float32)
        out_ref[:, hh * vhead:] = ordered.astype(jnp.bfloat16)


def merge_kernel(dims, scal_ref, *refs):
    hh, vhead, count = dims
    out_ref = refs[-1]
    for parity in range(GROUP):
        blocks = [refs[s] for s in range(count) if s % GROUP == parity]
        logs = []
        for b in blocks:
            packed = b[:, hh * vhead:].astype(jnp.float32)
            logs.append(packed[:, :hh] + packed[:, hh:2 * hh] + packed[:, 2 * hh:3 * hh])
        top = functools.reduce(jnp.maximum, logs)
        weights = [jnp.exp2(v - top) for v in logs]
        total = sum(weights[1:], weights[0])
        weights = [w / total for w in weights]
        base = scal_ref[parity] * (hh * vhead)
        for h in range(hh):
            cols = slice(h * vhead, (h + 1) * vhead)
            value = sum(w[:, h:h + 1] * b[:, cols].astype(jnp.float32) for w, b in zip(weights, blocks))
            out_ref[:, pl.ds(pl.multiple_of(base + h * vhead, vhead), vhead)] = value.astype(jnp.bfloat16)


def on_device(
    q_nope, q_rope, cache_tiles, absorb_keys, absorb_values, page_counts, query_token, query_offsets, members, devices
):
    member = lax.axis_index("pages")
    lane = lax.axis_index("heads") % LANES
    heads_here, nope, latent = absorb_keys.shape
    vhead = absorb_values.shape[2]
    local_rows = q_nope.shape[0]
    rope = q_rope.shape[1] // heads_here
    full = cache_tiles.shape[1]
    slots = cache_tiles.shape[0] // PAGE
    rows = local_rows * members
    hh = heads_here // GROUP
    hb = min(HEADS_STEP, hh)
    mine = member % GROUP

    def over_pages(x, shift):
        return lax.ppermute(x, "pages", [(i, (i + shift) % members) for i in range(members)])

    def over_heads(x, bit):
        return lax.ppermute(x, "heads", [(i, i ^ bit) for i in range(devices)])

    sub = PAGE // LANES
    quarter = lax.dynamic_slice_in_dim(cache_tiles.reshape(slots, LANES, sub, full), lane, 1, axis=1)
    quarter = quarter.reshape(slots * sub, full)
    part0 = lax.ppermute(quarter, "pages", [(i, i ^ 1) for i in range(members)])
    part1 = over_heads(part0, 2)
    part2 = over_heads(part0, 1)
    part3 = over_heads(part1, 1)

    def share(which):
        return jnp.concatenate(
            [
                lax.dynamic_slice_in_dim(q_nope, which * hh * nope, hh * nope, axis=1),
                lax.dynamic_slice_in_dim(q_rope, which * hh * rope, hh * rope, axis=1),
            ],
            axis=1,
        )

    shares = [share((mine + s) % GROUP) for s in range(GROUP)]
    blocks = [shares[0]] + [over_pages(shares[s % GROUP], s) for s in range(1, members)]
    queries = jnp.concatenate(blocks, axis=0)
    sources = (member - jnp.arange(members)) % members
    row_token = query_token.reshape(members, local_rows)[sources].reshape(rows)
    limits = query_offsets[row_token]

    prefix = jnp.cumsum(page_counts) - page_counts
    partner = member ^ 1
    scalars = jnp.stack(
        [page_counts[member], prefix[member], page_counts[partner], prefix[partner], mine]
        + [lane, lane ^ 2, lane ^ 1, lane ^ 3]
    ).astype(jnp.int32)

    whole = lambda *shape: pl.BlockSpec(shape, lambda i, s: (0,) * len(shape))
    packed = hh * vhead + 128
    out = pl.pallas_call(
        functools.partial(attend_kernel, (hh, hb, nope, rope, latent, vhead, rows)),
        out_shape=jax.ShapeDtypeStruct((rows, packed), jnp.bfloat16),
        grid_spec=pltpu.PrefetchScalarGridSpec(
            num_scalar_prefetch=1,
            grid=(hh // hb,),
            in_specs=[
                whole(rows, hh * (nope + rope)),
                whole(1, rows),
                whole(rows, 1),
                whole(slots * PAGE, full),
                whole(slots * sub, full),
                whole(slots * sub, full),
                whole(slots * sub, full),
                whole(slots * sub, full),
                pl.BlockSpec((hb, nope, latent), lambda i, s: (s[4] * (hh // hb) + i, 0, 0)),
                pl.BlockSpec((hb, latent, vhead), lambda i, s: (s[4] * (hh // hb) + i, 0, 0)),
            ],
            out_specs=whole(rows, packed),
            scratch_shapes=[
                pltpu.VMEM((hb * rows, full), jnp.bfloat16),
                pltpu.VMEM((hb * rows, 1), jnp.float32),
                pltpu.VMEM((hb * rows, 1), jnp.float32),
                pltpu.VMEM((hb * rows, latent), jnp.float32),
                pltpu.VMEM((rows, 128), jnp.float32),
            ],
        ),
        compiler_params=pltpu.CompilerParams(dimension_semantics=("arbitrary",), vmem_limit_bytes=48 << 20),
        name="attend",
    )(scalars, queries, row_token[None, :], limits[:, None], cache_tiles, part0, part1, part2, part3,
      absorb_keys, absorb_values)

    def to_owner(shift):
        return lax.dynamic_slice_in_dim(out, ((member + shift) % members) * local_rows, local_rows, axis=0)

    arrived = [to_owner(0)] + [over_pages(to_owner(s), s) for s in range(1, members)]
    homes = jnp.stack([(mine + s) % GROUP for s in range(GROUP)]).astype(jnp.int32)
    return pl.pallas_call(
        functools.partial(merge_kernel, (hh, vhead, members)),
        out_shape=jax.ShapeDtypeStruct((local_rows, heads_here * vhead), jnp.bfloat16),
        grid_spec=pltpu.PrefetchScalarGridSpec(
            num_scalar_prefetch=1,
            grid=(1,),
            in_specs=[whole(local_rows, packed)] * members,
            out_specs=whole(local_rows, heads_here * vhead),
        ),
        name="merge",
    )(homes, *arrived)


def solution(mesh):
    in_specs = (
        P(("groups", "pages"), "heads"),
        P(("groups", "pages"), "heads"),
        P(("groups", "pages"), None),
        P("heads", None, None),
        P("heads", None, None),
        P("groups"),
        P("groups"),
        P("groups"),
    )
    body = functools.partial(on_device, members=mesh.shape["pages"], devices=mesh.shape["heads"])
    return jax.shard_map(
        body, mesh=mesh, in_specs=in_specs, out_specs=P(("groups", "pages"), "heads"), check_vma=False
    )
```

```python
import functools

import jax
import jax.numpy as jnp
from jax import lax
from jax.experimental import pallas as pl
from jax.experimental.pallas import tpu as pltpu
from jax.sharding import PartitionSpec as P

PAGE = 64
GROUP = 2
LANES = 4
BLOCK_PAGES = 8
HEADS_STEP = 4
CHUNKS = 2

FLOOR = -1e30
FAR = 2**30
LOG2E = 1.4426950408889634


def pack_kernel(dims, nope_ref, rope_ref, cache_ref, share0_ref, share1_ref, quarter_ref, sems):
    nope_width, rope_width, quarter_cols = dims
    mine = lax.axis_index("pages") % GROUP
    lane = lax.axis_index("heads") % LANES
    copies = [
        pltpu.make_async_copy(
            cache_ref.at[:, pl.ds(pl.multiple_of(lane * quarter_cols, 128), quarter_cols)], quarter_ref, sems.at[0]
        )
    ]
    for e, share in enumerate((share0_ref, share1_ref)):
        which = (mine + e) % GROUP
        for j, (ref, width, at) in enumerate(((nope_ref, nope_width, 0), (rope_ref, rope_width, nope_width))):
            copies.append(
                pltpu.make_async_copy(
                    ref.at[:, pl.ds(pl.multiple_of(which * width, 128), width)],
                    share.at[:, pl.ds(at, width)],
                    sems.at[1 + 2 * e + j],
                )
            )
    for c in copies:
        c.start()
    for c in copies:
        c.wait()


def attend_kernel(dims, counts_ref, tok_ref, off_ref, *refs):
    members, first, hc, hh, hb, nope, rope, latent, vhead, rows, slots = dims
    q_refs, refs = refs[:members], refs[members:]
    part_refs, refs = refs[:LANES], refs[LANES:]
    own_ref, keys_hbm, values_hbm = refs[:3]
    out_refs, refs = refs[3:3 + members], refs[3 + members:]
    tiles, wk, wv, bias, qs, sbuf, mx, den, acc, lse, sems = refs
    local_rows = rows // members
    block = BLOCK_PAGES * PAGE
    cols = slots * PAGE
    scale2 = (nope + rope) ** (-0.5) * LOG2E
    steps = hc // hb
    member = lax.axis_index("pages")
    lane_id = lax.axis_index("heads") % LANES
    partner = member ^ 1
    mine = member % GROUP

    own_copy = pltpu.make_async_copy(own_ref, tiles.at[:, pl.ds(0, cols)], sems.at[0])
    own_copy.start()
    weight_copies = []
    for g in range(steps):
        at = pl.ds(mine * hh + first + g * hb, hb)
        pair = (
            pltpu.make_async_copy(keys_hbm.at[at], wk.at[pl.ds(g * hb, hb)], sems.at[1 + 2 * g]),
            pltpu.make_async_copy(values_hbm.at[at], wv.at[pl.ds(g * hb, hb)], sems.at[2 + 2 * g]),
        )
        for c in pair:
            c.start()
        weight_copies.append(pair)

    token = pltpu.roll(
        jnp.broadcast_to(tok_ref[...], (8, rows)), lax.rem(rows - member * local_rows, rows), axis=1
    )[:1]
    token_down = jnp.transpose(jnp.broadcast_to(token, (rows, rows)).astype(jnp.float32)).astype(jnp.int32)
    across = lax.broadcasted_iota(jnp.int32, (rows, rows), 1)
    down = lax.broadcasted_iota(jnp.int32, (rows, rows), 0)
    limit = jnp.max(jnp.where(token_down == across, off_ref[...], 0), axis=1, keepdims=True)
    owner = lax.rem(member - down // local_rows + members, members)
    order = (jnp.broadcast_to(token, (rows, rows)) == owner * local_rows + lax.rem(down, local_rows)).astype(
        jnp.bfloat16
    )

    quarter_cols = cols // LANES
    for ref, flip in zip(part_refs, (0, 2, 1, 3)):
        at = pl.multiple_of(cols + (lane_id ^ flip) * quarter_cols, 128)
        tiles[:, pl.ds(at, quarter_cols)] = ref[...]
    before = lambda who: lax.fori_loop(0, who, lambda i, total: total + counts_ref[i], jnp.int32(0))
    own_live, part_live = counts_ref[member], counts_ref[partner]
    own_base, part_base = before(member) * PAGE, before(partner) * PAGE
    own_blocks = (own_live + BLOCK_PAGES - 1) // BLOCK_PAGES
    blocks = own_blocks + (part_live + BLOCK_PAGES - 1) // BLOCK_PAGES

    def column(b):
        return pl.multiple_of(jnp.where(b < own_blocks, b * block, cols + (b - own_blocks) * block), 128)

    spot = lax.broadcasted_iota(jnp.int32, (1, block), 1)

    def fill_bias(b, carry):
        own = b < own_blocks
        inside = jnp.where(own, b, b - own_blocks) * block + spot
        live = jnp.where(own, own_live, part_live) * PAGE
        positions = jnp.where(inside < live, jnp.where(own, own_base, part_base) + inside, FAR)
        bias[:, pl.ds(pl.multiple_of(b * block, 128), block)] = jnp.where(positions < limit, 0.0, FLOOR)
        return carry

    lax.fori_loop(0, blocks, fill_bias, 0)
    lse[...] = jnp.zeros_like(lse)
    queries = [jnp.concatenate([q[:, (first + h) * nope:(first + h + 1) * nope] for q in q_refs], axis=0)
               for h in range(hc)]
    own_copy.wait()

    def absorb(g):
        slot = g % 2
        weight_copies[g][0].wait()
        for e in range(hb):
            h = g * hb + e
            lat = jnp.dot(queries[h], wk[h], preferred_element_type=jnp.float32)
            qs[slot, e * rows:(e + 1) * rows, :latent] = lat.astype(jnp.bfloat16)
        for e in range(0, hb, 2):
            at = hh * nope + (first + g * hb + e) * rope
            both = jnp.concatenate([q[:, at:at + 2 * rope] for q in q_refs], axis=0)
            for i in range(2):
                qs[slot, (e + i) * rows:(e + i + 1) * rows, latent:] = both[:, i * rope:(i + 1) * rope]
        mx[slot] = jnp.full(mx.shape[1:], FLOOR, jnp.float32)

    def score(g, b):
        slot = g % 2
        scores = jnp.dot(qs[slot], tiles[:, pl.ds(column(b), block)], preferred_element_type=jnp.float32)
        at = pl.multiple_of(b * block, 128)
        shut = bias[:, pl.ds(at, block)]
        for e in range(hb):
            part = slice(e * rows, (e + 1) * rows)
            value = scores[part] + shut
            sbuf[slot, part, pl.ds(at, block)] = value
            top = functools.reduce(jnp.maximum, [value[:, i:i + 128] for i in range(0, block, 128)])
            mx[slot, part] = jnp.maximum(mx[slot, part], top)

    def gather(g, b, top):
        slot = g % 2
        at = pl.multiple_of(b * block, 128)
        weights = jnp.exp2((sbuf[slot, :, pl.ds(at, block)] - top) * scale2)
        den[...] += functools.reduce(jnp.add, [weights[:, i:i + 128] for i in range(0, block, 128)])
        acc[...] += lax.dot_general(
            weights.astype(jnp.bfloat16),
            tiles[:latent, pl.ds(column(b), block)],
            (((1,), (1,)), ((), ())),
            preferred_element_type=jnp.float32,
        )

    lane = lax.broadcasted_iota(jnp.int32, (rows, 128), 1)

    def finish(g, top):
        weight_copies[g][1].wait()
        total = jnp.sum(den[...], axis=1, keepdims=True)
        seen = top > 0.5 * FLOOR
        total = jnp.where(seen, total, 1.0)
        latent_out = (acc[...] * jnp.where(seen, 1.0 / total, 0.0)).astype(jnp.bfloat16)
        logs = jnp.where(seen, top * scale2 + jnp.log2(total), FLOOR)
        for e in range(hb):
            h = g * hb + e
            part = slice(e * rows, (e + 1) * rows)
            value = jnp.dot(latent_out[part], wv[h], preferred_element_type=jnp.float32).astype(jnp.bfloat16)
            value = jnp.dot(order, value, preferred_element_type=jnp.float32).astype(jnp.bfloat16)
            for s in range(members):
                out_refs[s][:, h * vhead:(h + 1) * vhead] = value[s * local_rows:(s + 1) * local_rows]
            full = logs[part]
            high = full.astype(jnp.bfloat16).astype(jnp.float32)
            middle = (full - high).astype(jnp.bfloat16).astype(jnp.float32)
            low = full - high - middle
            lse[...] = jnp.where(lane == h, high, jnp.where(lane == hc + h, middle,
                                 jnp.where(lane == 2 * hc + h, low, lse[...])))

    top = None
    for g in range(steps + 1):
        if g < steps:
            absorb(g)
        if g > 0:
            den[...] = jnp.zeros_like(den)
            acc[...] = jnp.zeros_like(acc)

        def body(b, carry, g=g, top=top):
            if g < steps:
                score(g, b)
            if g > 0:
                gather(g - 1, b, top)
            return carry

        lax.fori_loop(0, blocks, body, 0)
        if g > 0:
            finish(g - 1, top)
        if g < steps:
            top = jnp.max(mx[g % 2], axis=1, keepdims=True)

    ordered = jnp.dot(order, lse[...].astype(jnp.bfloat16), preferred_element_type=jnp.float32).astype(jnp.bfloat16)
    for s in range(members):
        out_refs[s][:, hc * vhead:] = ordered[s * local_rows:(s + 1) * local_rows]


def merge_kernel(dims, *refs):
    hc, vhead, members, chunks = dims
    out_ref = refs[-1]
    mine = lax.axis_index("pages") % GROUP
    for c in range(chunks):
        for parity in range(GROUP):
            parts = [refs[c * members + s] for s in range(members) if s % GROUP == parity]
            logs = []
            for b in parts:
                packed = b[:, hc * vhead:].astype(jnp.float32)
                logs.append(packed[:, :hc] + packed[:, hc:2 * hc] + packed[:, 2 * hc:3 * hc])
            top = functools.reduce(jnp.maximum, logs)
            weights = [jnp.exp2(v - top) for v in logs]
            total = functools.reduce(jnp.add, weights)
            weights = [w / total for w in weights]
            base = (lax.rem(mine + parity, GROUP) * chunks + c) * (hc * vhead)
            for h in range(hc):
                cols = slice(h * vhead, (h + 1) * vhead)
                value = functools.reduce(
                    jnp.add, [w[:, h:h + 1] * b[:, cols].astype(jnp.float32) for w, b in zip(weights, parts)]
                )
                out_ref[:, pl.ds(pl.multiple_of(base + h * vhead, 128), vhead)] = value.astype(jnp.bfloat16)


def on_device(
    q_nope, q_rope, cache_tiles, absorb_keys, absorb_values, page_counts, query_token, query_offsets, members, devices
):
    heads_here, nope, latent = absorb_keys.shape
    vhead = absorb_values.shape[2]
    local_rows = q_nope.shape[0]
    rope = q_rope.shape[1] // heads_here
    full = cache_tiles.shape[1]
    slots = cache_tiles.shape[0] // PAGE
    cols = slots * PAGE
    rows = local_rows * members
    hh = heads_here // GROUP
    chunks = min(CHUNKS, hh // 2)
    hc = hh // chunks
    hb = min(HEADS_STEP, hc)
    hbm = pl.BlockSpec(memory_space=pltpu.HBM)
    vmem = pl.BlockSpec(memory_space=pltpu.VMEM)
    bf16 = jnp.bfloat16

    def over_pages(x, s):
        return lax.ppermute(x, "pages", [(i, (i - s) % members) for i in range(members)])

    def over_heads(x, bit):
        return lax.ppermute(x, "heads", [(i, i ^ bit) for i in range(devices)])

    turned = cache_tiles.T
    share0, share1, quarter = pl.pallas_call(
        functools.partial(pack_kernel, (hh * nope, hh * rope, cols // LANES)),
        out_shape=[jax.ShapeDtypeStruct((local_rows, hh * (nope + rope)), bf16)] * 2
        + [jax.ShapeDtypeStruct((full, cols // LANES), bf16)],
        in_specs=[hbm] * 3,
        out_specs=[vmem] * 3,
        scratch_shapes=[pltpu.SemaphoreType.DMA((5,))],
        name="pack",
    )(q_nope, q_rope, turned)

    part0 = lax.ppermute(quarter, "pages", [(i, i ^ 1) for i in range(members)])
    shares = (share0, share1)
    queries = [share0] + [over_pages(shares[s % GROUP], s) for s in range(1, members)]
    part1 = over_heads(part0, 2)
    part2 = over_heads(part0, 1)
    part3 = over_heads(part1, 1)

    packed = hc * vhead + 128
    block = BLOCK_PAGES * PAGE
    most = 2 * (-(-cols // block))
    arrived = []
    for c in range(chunks):
        outs = pl.pallas_call(
            functools.partial(
                attend_kernel, (members, c * hc, hc, hh, hb, nope, rope, latent, vhead, rows, slots)
            ),
            out_shape=[jax.ShapeDtypeStruct((local_rows, packed), bf16)] * members,
            in_specs=[pl.BlockSpec(memory_space=pltpu.SMEM)] + [vmem] * (2 + members + LANES) + [hbm] * 3,
            out_specs=[vmem] * members,
            scratch_shapes=[
                pltpu.VMEM((full, 2 * cols), bf16),
                pltpu.VMEM((hc, nope, latent), bf16),
                pltpu.VMEM((hc, latent, vhead), bf16),
                pltpu.VMEM((rows, most * block), jnp.float32),
                pltpu.VMEM((2, hb * rows, full), bf16),
                pltpu.VMEM((2, hb * rows, most * block), jnp.float32),
                pltpu.VMEM((2, hb * rows, 128), jnp.float32),
                pltpu.VMEM((hb * rows, 128), jnp.float32),
                pltpu.VMEM((hb * rows, latent), jnp.float32),
                pltpu.VMEM((rows, 128), jnp.float32),
                pltpu.SemaphoreType.DMA((1 + 2 * (hc // hb),)),
            ],
            compiler_params=pltpu.CompilerParams(vmem_limit_bytes=56 << 20),
            cost_estimate=pl.CostEstimate(flops=8 * 10**9 // chunks, bytes_accessed=8 * 10**6, transcendentals=0),
            name=f"attend{c}",
        )(page_counts, query_token[None, :], query_offsets[None, :], *queries, part0, part1, part2, part3,
          turned, absorb_keys, absorb_values)
        arrived += [outs[0]] + [over_pages(outs[s], s) for s in range(1, members)]

    return pl.pallas_call(
        functools.partial(merge_kernel, (hc, vhead, members, chunks)),
        out_shape=jax.ShapeDtypeStruct((local_rows, heads_here * vhead), bf16),
        in_specs=[vmem] * (members * chunks),
        out_specs=vmem,
        name="merge",
    )(*arrived)


def solution(mesh):
    in_specs = (
        P(("groups", "pages"), "heads"),
        P(("groups", "pages"), "heads"),
        P(("groups", "pages"), None),
        P("heads", None, None),
        P("heads", None, None),
        P("groups"),
        P("groups"),
        P("groups"),
    )
    body = functools.partial(on_device, members=mesh.shape["pages"], devices=mesh.shape["heads"])
    return jax.shard_map(
        body, mesh=mesh, in_specs=in_specs, out_specs=P(("groups", "pages"), "heads"), check_vma=False
    )
```

```python
import functools

import jax
import jax.numpy as jnp
from jax import lax
from jax.experimental import pallas as pl
from jax.experimental.pallas import tpu as pltpu
from jax.sharding import PartitionSpec as P


PAGE = 64
GROUP = 2
LANES = 4
BLOCK_PAGES = 8
HEADS_STEP = 4
CHUNKS = 2


FLOOR = -1e30
FAR = 2**30
LOG2E = 1.4426950408889634


def pack_kernel(dims, nope_ref, rope_ref, cache_ref, *refs):
    nope_width, rope_width, quarter_cols, chunks = dims
    outs, sems = refs[:-1], refs[-1]
    mine = lax.axis_index("pages") % GROUP
    lane = lax.axis_index("heads") % LANES
    copies = [
        pltpu.make_async_copy(
            cache_ref.at[:, pl.ds(pl.multiple_of(lane * quarter_cols, 128), quarter_cols)], outs[0], sems.at[0]
        )
    ]
    for c in range(chunks):
        for e in range(GROUP):
            which = ((mine + e) % GROUP) * chunks + c
            for ref, width, at in ((nope_ref, nope_width, 0), (rope_ref, rope_width, nope_width)):
                copies.append(
                    pltpu.make_async_copy(
                        ref.at[:, pl.ds(pl.multiple_of(which * width, 128), width)],
                        outs[1 + c * GROUP + e].at[:, pl.ds(at, width)],
                        sems.at[len(copies)],
                    )
                )
    for c in copies:
        c.start()
    for c in copies:
        c.wait()


def prepare_kernel(dims, tok_ref, off_ref, limit_ref, order_ref):
    members, rows = dims
    local_rows = rows // members
    member = lax.axis_index("pages")
    token = pltpu.roll(
        jnp.broadcast_to(tok_ref[...], (8, rows)), lax.rem(rows - member * local_rows, rows), axis=1
    )[:1]
    token_down = jnp.transpose(jnp.broadcast_to(token, (rows, rows)).astype(jnp.float32)).astype(jnp.int32)
    across = lax.broadcasted_iota(jnp.int32, (rows, rows), 1)
    down = lax.broadcasted_iota(jnp.int32, (rows, rows), 0)
    limit = jnp.max(jnp.where(token_down == across, off_ref[...], 0), axis=1, keepdims=True)
    limit_ref[...] = jnp.broadcast_to(limit, limit_ref.shape)
    owner = lax.rem(member - down // local_rows + members, members)
    order_ref[...] = (
        jnp.broadcast_to(token, (rows, rows)) == owner * local_rows + lax.rem(down, local_rows)
    ).astype(jnp.bfloat16)


def attend_kernel(dims, counts_ref, limit_ref, order_ref, *refs):
    members, first, hc, hh, hb, nope, rope, latent, vhead, rows, slots = dims
    q_refs, refs = refs[:members], refs[members:]
    part_refs, refs = refs[:LANES], refs[LANES:]
    own_ref, keys_hbm, values_hbm = refs[:3]
    out_refs, refs = refs[3:3 + members], refs[3 + members:]
    tiles, wk, wv, bias, qs, sbuf, mx, den, acc, lse, sems, tile_sems = refs
    local_rows = rows // members
    block = BLOCK_PAGES * PAGE
    cols = slots * PAGE
    quarter_cols = cols // LANES
    scale2 = (nope + rope) ** (-0.5) * LOG2E
    steps = hc // hb
    member = lax.axis_index("pages")
    lane_id = lax.axis_index("heads") % LANES
    partner = member ^ 1
    mine = member % GROUP

    weight_copies = []
    for g in range(steps):
        at = pl.ds(mine * hh + first + g * hb, hb)
        weight_copies.append((
            pltpu.make_async_copy(keys_hbm.at[at], wk.at[pl.ds(g * hb, hb)], sems.at[2 * g]),
            pltpu.make_async_copy(values_hbm.at[at], wv.at[pl.ds(g * hb, hb)], sems.at[1 + 2 * g]),
        ))
    tile_copies = [pltpu.make_async_copy(own_ref, tiles.at[:, pl.ds(0, cols)], tile_sems.at[0])]
    for i, (ref, flip) in enumerate(zip(part_refs, (0, 2, 1, 3))):
        at = pl.multiple_of(cols + (lane_id ^ flip) * quarter_cols, 128)
        tile_copies.append(pltpu.make_async_copy(ref, tiles.at[:, pl.ds(at, quarter_cols)], tile_sems.at[1 + i]))
    weight_copies[0][0].start()
    for c in tile_copies:
        c.start()
    weight_copies[0][1].start()
    for pair in weight_copies[1:]:
        for c in pair:
            c.start()

    before = lambda who: lax.fori_loop(0, who, lambda i, total: total + counts_ref[i], jnp.int32(0))
    limit = limit_ref[:, :1]
    order = order_ref[...]
    own_live, part_live = counts_ref[member], counts_ref[partner]
    own_base, part_base = before(member) * PAGE, before(partner) * PAGE
    own_blocks = (own_live + BLOCK_PAGES - 1) // BLOCK_PAGES
    blocks = own_blocks + (part_live + BLOCK_PAGES - 1) // BLOCK_PAGES

    def column(b):
        return pl.multiple_of(jnp.where(b < own_blocks, b * block, cols + (b - own_blocks) * block), 128)

    spot = lax.broadcasted_iota(jnp.int32, (1, block), 1)

    def fill_bias(b, carry):
        own = b < own_blocks
        inside = jnp.where(own, b, b - own_blocks) * block + spot
        live = jnp.where(own, own_live, part_live) * PAGE
        positions = jnp.where(inside < live, jnp.where(own, own_base, part_base) + inside, FAR)
        bias[:, pl.ds(pl.multiple_of(b * block, 128), block)] = jnp.where(positions < limit, 0.0, FLOOR)
        return carry

    lax.fori_loop(0, blocks, fill_bias, 0)
    lse[...] = jnp.zeros_like(lse)

    def absorb(g):
        slot = g % 2
        weight_copies[g][0].wait()
        for e in range(hb):
            h = g * hb + e
            query = jnp.concatenate([q[:, h * nope:(h + 1) * nope] for q in q_refs], axis=0)
            lat = jnp.dot(query, wk[h], preferred_element_type=jnp.float32)
            qs[slot, e * rows:(e + 1) * rows, :latent] = lat.astype(jnp.bfloat16)
        for e in range(0, hb, 2):
            at = hc * nope + (g * hb + e) * rope
            both = jnp.concatenate([q[:, at:at + 2 * rope] for q in q_refs], axis=0)
            for i in range(2):
                qs[slot, (e + i) * rows:(e + i + 1) * rows, latent:] = both[:, i * rope:(i + 1) * rope]
        mx[slot] = jnp.full(mx.shape[1:], FLOOR, jnp.float32)

    def score(g, b):
        slot = g % 2
        scores = jnp.dot(qs[slot], tiles[:, pl.ds(column(b), block)], preferred_element_type=jnp.float32)
        at = pl.multiple_of(b * block, 128)
        shut = bias[:, pl.ds(at, block)]
        for e in range(hb):
            part = slice(e * rows, (e + 1) * rows)
            value = scores[part] + shut
            sbuf[slot, part, pl.ds(at, block)] = value
            top = functools.reduce(jnp.maximum, [value[:, i:i + 128] for i in range(0, block, 128)])
            mx[slot, part] = jnp.maximum(mx[slot, part], top)

    def gather(g, b, top):
        slot = g % 2
        at = pl.multiple_of(b * block, 128)
        weights = jnp.exp2((sbuf[slot, :, pl.ds(at, block)] - top) * scale2)
        den[...] += functools.reduce(jnp.add, [weights[:, i:i + 128] for i in range(0, block, 128)])
        acc[...] += lax.dot_general(
            weights.astype(jnp.bfloat16),
            tiles[:latent, pl.ds(column(b), block)],
            (((1,), (1,)), ((), ())),
            preferred_element_type=jnp.float32,
        )

    lane = lax.broadcasted_iota(jnp.int32, (rows, 128), 1)

    def finish(g, top):
        weight_copies[g][1].wait()
        total = jnp.sum(den[...], axis=1, keepdims=True)
        seen = top > 0.5 * FLOOR
        total = jnp.where(seen, total, 1.0)
        latent_out = (acc[...] * jnp.where(seen, 1.0 / total, 0.0)).astype(jnp.bfloat16)
        logs = jnp.where(seen, top * scale2 + jnp.log2(total), FLOOR)
        for e in range(hb):
            h = g * hb + e
            part = slice(e * rows, (e + 1) * rows)
            value = jnp.dot(latent_out[part], wv[h], preferred_element_type=jnp.float32).astype(jnp.bfloat16)
            value = jnp.dot(order, value, preferred_element_type=jnp.float32).astype(jnp.bfloat16)
            for s in range(members):
                out_refs[s][:, h * vhead:(h + 1) * vhead] = value[s * local_rows:(s + 1) * local_rows]
            full = logs[part]
            high = full.astype(jnp.bfloat16).astype(jnp.float32)
            middle = (full - high).astype(jnp.bfloat16).astype(jnp.float32)
            low = full - high - middle
            lse[...] = jnp.where(lane == h, high, jnp.where(lane == hc + h, middle,
                                 jnp.where(lane == 2 * hc + h, low, lse[...])))

    top = None
    for g in range(steps + 1):
        if g < steps:
            absorb(g)
        if g == 0:
            for c in tile_copies:
                c.wait()
        if g > 0:
            den[...] = jnp.zeros_like(den)
            acc[...] = jnp.zeros_like(acc)

        def body(b, carry, g=g, top=top):
            if g < steps:
                score(g, b)
            if g > 0:
                gather(g - 1, b, top)
            return carry

        lax.fori_loop(0, blocks, body, 0)
        if g > 0:
            finish(g - 1, top)
        if g < steps:
            top = jnp.max(mx[g % 2], axis=1, keepdims=True)

    ordered = jnp.dot(order, lse[...].astype(jnp.bfloat16), preferred_element_type=jnp.float32).astype(jnp.bfloat16)
    for s in range(members):
        out_refs[s][:, hc * vhead:] = ordered[s * local_rows:(s + 1) * local_rows]


def merge_kernel(dims, *refs):
    hc, vhead, members, chunks = dims
    out_ref = refs[-1]
    mine = lax.axis_index("pages") % GROUP
    for c in range(chunks):
        for parity in range(GROUP):
            parts = [refs[c * members + s] for s in range(members) if s % GROUP == parity]
            logs = []
            for b in parts:
                packed = b[:, hc * vhead:].astype(jnp.float32)
                logs.append(packed[:, :hc] + packed[:, hc:2 * hc] + packed[:, 2 * hc:3 * hc])
            top = functools.reduce(jnp.maximum, logs)
            weights = [jnp.exp2(v - top) for v in logs]
            total = functools.reduce(jnp.add, weights)
            weights = [w / total for w in weights]
            base = (lax.rem(mine + parity, GROUP) * chunks + c) * (hc * vhead)
            for h in range(hc):
                cols = slice(h * vhead, (h + 1) * vhead)
                value = functools.reduce(
                    jnp.add, [w[:, h:h + 1] * b[:, cols].astype(jnp.float32) for w, b in zip(weights, parts)]
                )
                out_ref[:, pl.ds(pl.multiple_of(base + h * vhead, 128), vhead)] = value.astype(jnp.bfloat16)


def on_device(
    q_nope, q_rope, cache_tiles, absorb_keys, absorb_values, page_counts, query_token, query_offsets, members, devices
):
    heads_here, nope, latent = absorb_keys.shape
    vhead = absorb_values.shape[2]
    local_rows = q_nope.shape[0]
    rope = q_rope.shape[1] // heads_here
    full = cache_tiles.shape[1]
    slots = cache_tiles.shape[0] // PAGE
    cols = slots * PAGE
    rows = local_rows * members
    hh = heads_here // GROUP
    chunks = min(CHUNKS, hh // 2)
    hc = hh // chunks
    hb = min(HEADS_STEP, hc)
    hbm = pl.BlockSpec(memory_space=pltpu.HBM)
    vmem = pl.BlockSpec(memory_space=pltpu.VMEM)
    bf16 = jnp.bfloat16

    def over_pages(x, s):
        return lax.ppermute(x, "pages", [(i, (i - s) % members) for i in range(members)])

    def over_heads(x, bit):
        return lax.ppermute(x, "heads", [(i, i ^ bit) for i in range(devices)])

    turned = cache_tiles.T
    quarter, *shares = pl.pallas_call(
        functools.partial(pack_kernel, (hc * nope, hc * rope, cols // LANES, chunks)),
        out_shape=[jax.ShapeDtypeStruct((full, cols // LANES), bf16)]
        + [jax.ShapeDtypeStruct((local_rows, hc * (nope + rope)), bf16)] * (GROUP * chunks),
        in_specs=[hbm] * 3,
        out_specs=[vmem] * (1 + GROUP * chunks),
        scratch_shapes=[pltpu.SemaphoreType.DMA((1 + 2 * GROUP * chunks,))],
        name="pack",
    )(q_nope, q_rope, turned)
    limits, order = pl.pallas_call(
        functools.partial(prepare_kernel, (members, rows)),
        out_shape=[jax.ShapeDtypeStruct((rows, 128), jnp.int32), jax.ShapeDtypeStruct((rows, rows), bf16)],
        in_specs=[vmem] * 2,
        out_specs=[vmem] * 2,
        name="prepare",
    )(query_token[None, :], query_offsets[None, :])

    part0 = lax.ppermute(quarter, "pages", [(i, i ^ 1) for i in range(members)])
    queries = []
    for c in range(chunks):
        own, other = shares[c * GROUP:(c + 1) * GROUP]
        sent = {}
        for s in sorted(range(1, members), key=lambda s: s % GROUP):
            sent[s] = over_pages((own, other)[s % GROUP], s)
        queries.append([own] + [sent[s] for s in range(1, members)])
    part1 = over_heads(part0, 2)
    part2 = over_heads(part0, 1)
    part3 = over_heads(part1, 1)

    packed = hc * vhead + 128
    block = BLOCK_PAGES * PAGE
    most = 2 * (-(-cols // block))
    arrived = []
    for c in range(chunks):
        outs = pl.pallas_call(
            functools.partial(
                attend_kernel, (members, c * hc, hc, hh, hb, nope, rope, latent, vhead, rows, slots)
            ),
            out_shape=[jax.ShapeDtypeStruct((local_rows, packed), bf16)] * members,
            in_specs=[pl.BlockSpec(memory_space=pltpu.SMEM)] + [vmem] * (2 + members) + [hbm] * (LANES + 3),
            out_specs=[vmem] * members,
            scratch_shapes=[
                pltpu.VMEM((full, 2 * cols), bf16),
                pltpu.VMEM((hc, nope, latent), bf16),
                pltpu.VMEM((hc, latent, vhead), bf16),
                pltpu.VMEM((rows, most * block), jnp.float32),
                pltpu.VMEM((2, hb * rows, full), bf16),
                pltpu.VMEM((2, hb * rows, most * block), jnp.float32),
                pltpu.VMEM((2, hb * rows, 128), jnp.float32),
                pltpu.VMEM((hb * rows, 128), jnp.float32),
                pltpu.VMEM((hb * rows, latent), jnp.float32),
                pltpu.VMEM((rows, 128), jnp.float32),
                pltpu.SemaphoreType.DMA((2 * (hc // hb),)),
                pltpu.SemaphoreType.DMA((1 + LANES,)),
            ],
            compiler_params=pltpu.CompilerParams(vmem_limit_bytes=56 << 20),
            cost_estimate=pl.CostEstimate(flops=8 * 10**9 // chunks, bytes_accessed=8 * 10**6, transcendentals=0),
        )(page_counts, limits, order, *queries[c], part0, part1, part2, part3,
          turned, absorb_keys, absorb_values)
        arrived.append(outs[0])
        for s in range(1, members):
            arrived.append(over_pages(outs[s], s))

    return pl.pallas_call(
        functools.partial(merge_kernel, (hc, vhead, members, chunks)),
        out_shape=jax.ShapeDtypeStruct((local_rows, heads_here * vhead), bf16),
        in_specs=[vmem] * (members * chunks),
        out_specs=vmem,
        name="merge",
    )(*arrived)


def solution(mesh):
    in_specs = (
        P(("groups", "pages"), "heads"),
        P(("groups", "pages"), "heads"),
        P(("groups", "pages"), None),
        P("heads", None, None),
        P("heads", None, None),
        P("groups"),
        P("groups"),
        P("groups"),
    )
    body = functools.partial(on_device, members=mesh.shape["pages"], devices=mesh.shape["heads"])
    return jax.shard_map(
        body, mesh=mesh, in_specs=in_specs, out_specs=P(("groups", "pages"), "heads"), check_vma=False
    )
```

```python
import functools

import jax
import jax.numpy as jnp
from jax import lax
from jax.experimental import pallas as pl
from jax.experimental.pallas import tpu as pltpu
from jax.sharding import PartitionSpec as P


PAGE = 64
GROUP = 2
LANES = 4
BLOCK_PAGES = 8
HEADS_STEP = 4
PIECES = 2
CHUNKS = 2


FLOOR = -1e30
FAR = 2**30
LOG2E = 1.4426950408889634


def pack_kernel(dims, nope_ref, rope_ref, cache_ref, *refs):
    nope_width, rope_width, quarter_cols, chunks = dims
    outs, sems = refs[:-1], refs[-1]
    mine = lax.axis_index("pages") % GROUP
    lane = lax.axis_index("heads") % LANES
    depth = cache_ref.shape[0] // PIECES
    copies = []
    for p in range(PIECES):
        copies.append(
            pltpu.make_async_copy(
                cache_ref.at[pl.ds(p * depth, depth), pl.ds(pl.multiple_of(lane * quarter_cols, 128), quarter_cols)],
                outs[p],
                sems.at[p],
            )
        )
    for c in range(chunks):
        for e in range(GROUP):
            which = ((mine + e) % GROUP) * chunks + c
            for ref, width, at in ((nope_ref, nope_width, 0), (rope_ref, rope_width, nope_width)):
                copies.append(
                    pltpu.make_async_copy(
                        ref.at[:, pl.ds(pl.multiple_of(which * width, 128), width)],
                        outs[PIECES + c * GROUP + e].at[:, pl.ds(at, width)],
                        sems.at[len(copies)],
                    )
                )
    for c in copies:
        c.start()
    for c in copies:
        c.wait()


def absorb_kernel(dims, tok_ref, off_ref, *refs):
    members, first, hc, hh, nope, rope, latent = dims
    q_refs, keys_hbm, qs_ref, limit_ref, wk, sem = refs[:members], *refs[members:]
    rows = limit_ref.shape[0]
    local_rows = rows // members
    member = lax.axis_index("pages")
    mine = member % GROUP
    copy = pltpu.make_async_copy(keys_hbm.at[pl.ds(mine * hh + first, hc)], wk, sem)
    copy.start()
    token = pltpu.roll(
        jnp.broadcast_to(tok_ref[...], (8, rows)), lax.rem(rows - member * local_rows, rows), axis=1
    )[:1]
    across = lax.broadcasted_iota(jnp.int32, (rows, rows), 1)
    down = lax.broadcasted_iota(jnp.int32, (rows, rows), 0)
    wanted = lax.rem(member - down // local_rows + members, members) * local_rows + lax.rem(down, local_rows)
    order = (jnp.broadcast_to(token, (rows, rows)) == wanted).astype(jnp.bfloat16)
    limit = jnp.max(jnp.where(across == wanted, off_ref[...], 0), axis=1, keepdims=True)
    limit_ref[...] = jnp.broadcast_to(limit, limit_ref.shape)
    copy.wait()
    for h in range(hc):
        query = jnp.concatenate([q[:, h * nope:(h + 1) * nope] for q in q_refs], axis=0)
        query = jnp.dot(order, query, preferred_element_type=jnp.float32).astype(jnp.bfloat16)
        lat = jnp.dot(query, wk[h], preferred_element_type=jnp.float32)
        qs_ref[h * rows:(h + 1) * rows, :latent] = lat.astype(jnp.bfloat16)
    for h in range(0, hc, 2):
        at = hc * nope + h * rope
        both = jnp.concatenate([q[:, at:at + 2 * rope] for q in q_refs], axis=0)
        both = jnp.dot(order, both, preferred_element_type=jnp.float32).astype(jnp.bfloat16)
        for i in range(2):
            qs_ref[(h + i) * rows:(h + i + 1) * rows, latent:] = both[:, i * rope:(i + 1) * rope]


def attend_kernel(dims, counts_ref, limit_ref, qs_hbm, *refs):
    members, first, hc, hh, hb, nope, rope, latent, vhead, rows, slots = dims
    part_refs, refs = refs[:LANES * PIECES], refs[LANES * PIECES:]
    own_ref, values_hbm = refs[:2]
    out_refs, refs = refs[2:2 + members], refs[2 + members:]
    tiles, wv, bias, qs, sbuf, mx, den, acc, lse, sems, own_sems, part_sems = refs
    local_rows = rows // members
    block = BLOCK_PAGES * PAGE
    cols = slots * PAGE
    quarter_cols = cols // LANES
    depth = (latent + rope) // PIECES
    scale2 = (nope + rope) ** (-0.5) * LOG2E
    steps = hc // hb
    group_rows = hb * rows
    member = lax.axis_index("pages")
    lane_id = lax.axis_index("heads") % LANES
    partner = member ^ 1
    mine = member % GROUP
    own_live, part_live = counts_ref[member], counts_ref[partner]
    own_blocks = (own_live + BLOCK_PAGES - 1) // BLOCK_PAGES
    part_blocks = (part_live + BLOCK_PAGES - 1) // BLOCK_PAGES
    blocks = own_blocks + part_blocks

    query_copies = [
        pltpu.make_async_copy(
            qs_hbm.at[pl.ds(g * group_rows, group_rows)], qs.at[pl.ds(g * group_rows, group_rows)], sems.at[g]
        )
        for g in range(steps)
    ]
    value_copy = pltpu.make_async_copy(values_hbm.at[pl.ds(mine * hh + first, hc)], wv, sems.at[steps])
    tile_copies = []
    for b in range(-(-cols // block)):
        at = pl.ds(b * block, min(block, cols - b * block))
        tile_copies.append((b < own_blocks, pltpu.make_async_copy(own_ref.at[:, at], tiles.at[:, at], own_sems.at[b])))
    for i, flip in enumerate((0, 2, 1, 3)):
        quarter = lane_id ^ flip
        at = pl.multiple_of(cols + quarter * quarter_cols, 128)
        for p in range(PIECES):
            tile_copies.append((
                quarter * quarter_cols < part_blocks * block,
                pltpu.make_async_copy(
                    part_refs[i * PIECES + p],
                    tiles.at[pl.ds(p * depth, depth), pl.ds(at, quarter_cols)],
                    part_sems.at[i * PIECES + p],
                ),
            ))
    query_copies[0].start()
    for used, copy in tile_copies:
        pl.when(used)(copy.start)
    for copy in query_copies[1:] + [value_copy]:
        copy.start()

    before = lambda who: lax.fori_loop(0, who, lambda i, total: total + counts_ref[i], jnp.int32(0))
    limit = limit_ref[:, :1]
    own_base, part_base = before(member) * PAGE, before(partner) * PAGE

    def column(b):
        return pl.multiple_of(jnp.where(b < own_blocks, b * block, cols + (b - own_blocks) * block), 128)

    spot = lax.broadcasted_iota(jnp.int32, (1, block), 1)

    def fill_bias(b, carry):
        own = b < own_blocks
        inside = jnp.where(own, b, b - own_blocks) * block + spot
        live = jnp.where(own, own_live, part_live) * PAGE
        positions = jnp.where(inside < live, jnp.where(own, own_base, part_base) + inside, FAR)
        bias[:, pl.ds(pl.multiple_of(b * block, 128), block)] = jnp.where(positions < limit, 0.0, FLOOR)
        return carry

    lax.fori_loop(0, blocks, fill_bias, 0)
    lse[...] = jnp.zeros_like(lse)

    def score(g, b):
        slot = g % 2
        scores = jnp.dot(qs[g * group_rows:(g + 1) * group_rows], tiles[:, pl.ds(column(b), block)], preferred_element_type=jnp.float32)
        at = pl.multiple_of(b * block, 128)
        shut = bias[:, pl.ds(at, block)]
        for e in range(hb):
            part = slice(e * rows, (e + 1) * rows)
            value = scores[part] + shut
            sbuf[slot, part, pl.ds(at, block)] = value
            top = functools.reduce(jnp.maximum, [value[:, i:i + 128] for i in range(0, block, 128)])
            mx[slot, part] = jnp.maximum(mx[slot, part], top)

    def gather(g, b, top):
        slot = g % 2
        at = pl.multiple_of(b * block, 128)
        weights = jnp.exp2((sbuf[slot, :, pl.ds(at, block)] - top) * scale2)
        den[...] += functools.reduce(jnp.add, [weights[:, i:i + 128] for i in range(0, block, 128)])
        acc[...] += lax.dot_general(
            weights.astype(jnp.bfloat16),
            tiles[:latent, pl.ds(column(b), block)],
            (((1,), (1,)), ((), ())),
            preferred_element_type=jnp.float32,
        )

    lane = lax.broadcasted_iota(jnp.int32, (rows, 128), 1)

    def finish(g, top):
        total = jnp.sum(den[...], axis=1, keepdims=True)
        seen = top > 0.5 * FLOOR
        total = jnp.where(seen, total, 1.0)
        share = jnp.where(seen, 1.0 / total, 0.0)
        logs = jnp.where(seen, top * scale2 + jnp.log2(total), FLOOR)
        for e in range(hb):
            h = g * hb + e
            part = slice(e * rows, (e + 1) * rows)
            value = jnp.dot(acc[part].astype(jnp.bfloat16), wv[h], preferred_element_type=jnp.float32)
            value = (value * share[part]).astype(jnp.bfloat16)
            for s in range(members):
                out_refs[s][:, h * vhead:(h + 1) * vhead] = value[s * local_rows:(s + 1) * local_rows]
            full = logs[part]
            high = full.astype(jnp.bfloat16).astype(jnp.float32)
            middle = (full - high).astype(jnp.bfloat16).astype(jnp.float32)
            low = full - high - middle
            lse[...] = jnp.where(lane == h, high, jnp.where(lane == hc + h, middle,
                                 jnp.where(lane == 2 * hc + h, low, lse[...])))

    top = None
    for g in range(steps + 1):
        if g < steps:
            query_copies[g].wait()
            mx[g % 2] = jnp.full(mx.shape[1:], FLOOR, jnp.float32)
        if g == 0:
            for used, copy in tile_copies:
                pl.when(used)(copy.wait)
        if g == 1:
            value_copy.wait()
        if g > 0:
            den[...] = jnp.zeros_like(den)
            acc[...] = jnp.zeros_like(acc)

        def body(b, carry, g=g, top=top):
            if g < steps:
                score(g, b)
            if g > 0:
                gather(g - 1, b, top)
            return carry

        lax.fori_loop(0, blocks, body, 0)
        if g > 0:
            finish(g - 1, top)
        if g < steps:
            top = jnp.max(mx[g % 2], axis=1, keepdims=True)

    for s in range(members):
        out_refs[s][:, hc * vhead:] = lse[s * local_rows:(s + 1) * local_rows].astype(jnp.bfloat16)


def attend_call(members, first, hc, hh, hb, nope, rope, latent, vhead, rows, slots, chunks):
    hbm = pl.BlockSpec(memory_space=pltpu.HBM)
    vmem = pl.BlockSpec(memory_space=pltpu.VMEM)
    bf16 = jnp.bfloat16
    full = latent + rope
    cols = slots * PAGE
    local_rows = rows // members
    packed = hc * vhead + 128
    block = BLOCK_PAGES * PAGE
    most = 2 * (-(-cols // block))
    return pl.pallas_call(
        functools.partial(
            attend_kernel, (members, first, hc, hh, hb, nope, rope, latent, vhead, rows, slots)
        ),
        out_shape=[jax.ShapeDtypeStruct((local_rows, packed), bf16)] * members,
        in_specs=[pl.BlockSpec(memory_space=pltpu.SMEM), vmem] + [hbm] * (1 + LANES * PIECES + 2),
        out_specs=[vmem] * members,
        scratch_shapes=[
            pltpu.VMEM((full, 2 * cols), bf16),
            pltpu.VMEM((hc, latent, vhead), bf16),
            pltpu.VMEM((rows, most * block), jnp.float32),
            pltpu.VMEM((hc * rows, full), bf16),
            pltpu.VMEM((2, hb * rows, most * block), jnp.float32),
            pltpu.VMEM((2, hb * rows, 128), jnp.float32),
            pltpu.VMEM((hb * rows, 128), jnp.float32),
            pltpu.VMEM((hb * rows, latent), jnp.float32),
            pltpu.VMEM((rows, 128), jnp.float32),
            pltpu.SemaphoreType.DMA((1 + hc // hb,)),
            pltpu.SemaphoreType.DMA((most // 2,)),
            pltpu.SemaphoreType.DMA((LANES * PIECES,)),
        ],
        compiler_params=pltpu.CompilerParams(vmem_limit_bytes=56 << 20),
        cost_estimate=pl.CostEstimate(flops=8 * 10**9 // chunks, bytes_accessed=8 * 10**6, transcendentals=0),
    )


def merge_kernel(dims, *refs):
    hc, vhead, members, chunks = dims
    out_ref = refs[-1]
    mine = lax.axis_index("pages") % GROUP
    for c in range(chunks):
        for parity in range(GROUP):
            parts = [refs[c * members + s] for s in range(members) if s % GROUP == parity]
            logs = []
            for b in parts:
                packed = b[:, hc * vhead:].astype(jnp.float32)
                logs.append(packed[:, :hc] + packed[:, hc:2 * hc] + packed[:, 2 * hc:3 * hc])
            top = functools.reduce(jnp.maximum, logs)
            weights = [jnp.exp2(v - top) for v in logs]
            total = functools.reduce(jnp.add, weights)
            weights = [w / total for w in weights]
            base = (lax.rem(mine + parity, GROUP) * chunks + c) * (hc * vhead)
            for h in range(hc):
                cols = slice(h * vhead, (h + 1) * vhead)
                value = functools.reduce(
                    jnp.add, [w[:, h:h + 1] * b[:, cols].astype(jnp.float32) for w, b in zip(weights, parts)]
                )
                out_ref[:, pl.ds(pl.multiple_of(base + h * vhead, 128), vhead)] = value.astype(jnp.bfloat16)


def on_device(
    q_nope, q_rope, cache_tiles, absorb_keys, absorb_values, page_counts, query_token, query_offsets, members, devices
):
    heads_here, nope, latent = absorb_keys.shape
    vhead = absorb_values.shape[2]
    local_rows = q_nope.shape[0]
    rope = q_rope.shape[1] // heads_here
    full = cache_tiles.shape[1]
    slots = cache_tiles.shape[0] // PAGE
    cols = slots * PAGE
    rows = local_rows * members
    hh = heads_here // GROUP
    chunks = min(CHUNKS, hh // 2)
    hc = hh // chunks
    hb = min(HEADS_STEP, hc)
    hbm = pl.BlockSpec(memory_space=pltpu.HBM)
    vmem = pl.BlockSpec(memory_space=pltpu.VMEM)
    bf16 = jnp.bfloat16

    def over_pages(x, s):
        return lax.ppermute(x, "pages", [(i, (i - s) % members) for i in range(members)])

    def over_heads(x, bit):
        return lax.ppermute(x, "heads", [(i, i ^ bit) for i in range(devices)])

    turned = cache_tiles.T
    packed = pl.pallas_call(
        functools.partial(pack_kernel, (hc * nope, hc * rope, cols // LANES, chunks)),
        out_shape=[jax.ShapeDtypeStruct((full // PIECES, cols // LANES), bf16)] * PIECES
        + [jax.ShapeDtypeStruct((local_rows, hc * (nope + rope)), bf16)] * (GROUP * chunks),
        in_specs=[hbm] * 3,
        out_specs=[vmem] * (PIECES + GROUP * chunks),
        scratch_shapes=[pltpu.SemaphoreType.DMA((PIECES + 2 * GROUP * chunks,))],
        name="pack",
    )(q_nope, q_rope, turned)
    pieces, shares = packed[:PIECES], packed[PIECES:]

    parts = [[None] * PIECES for _ in range(LANES)]
    for p in range(PIECES):
        parts[0][p] = lax.ppermute(pieces[p], "pages", [(i, i ^ 1) for i in range(members)])
        parts[1][p] = over_heads(parts[0][p], 2)
        parts[2][p] = over_heads(parts[0][p], 1)
        parts[3][p] = over_heads(parts[1][p], 1)
    parts = [p for part in parts for p in part]
    absorbed = []
    for c in range(chunks):
        own, other = shares[c * GROUP:(c + 1) * GROUP]
        blocks = [own]
        for s in range(1, members):
            blocks.append(over_pages((own, other)[s % GROUP], s))
        absorbed.append(pl.pallas_call(
            functools.partial(absorb_kernel, (members, c * hc, hc, hh, nope, rope, latent)),
            out_shape=[
                jax.ShapeDtypeStruct((hc * rows, full), bf16),
                jax.ShapeDtypeStruct((rows, 128), jnp.int32),
            ],
            in_specs=[vmem] * (2 + members) + [hbm],
            out_specs=[vmem] * 2,
            scratch_shapes=[pltpu.VMEM((hc, nope, latent), bf16), pltpu.SemaphoreType.DMA(())],
        )(query_token[None, :], query_offsets[None, :], *blocks, absorb_keys))

    arrived = []
    for c in range(chunks):
        outs = attend_call(
            members, c * hc, hc, hh, hb, nope, rope, latent, vhead, rows, slots, chunks
        )(page_counts, absorbed[c][1], absorbed[c][0], *parts, turned, absorb_values)
        arrived.append(outs[0])
        for s in range(1, members):
            arrived.append(over_pages(outs[s], s))

    return pl.pallas_call(
        functools.partial(merge_kernel, (hc, vhead, members, chunks)),
        out_shape=jax.ShapeDtypeStruct((local_rows, heads_here * vhead), bf16),
        in_specs=[vmem] * (members * chunks),
        out_specs=vmem,
        name="merge",
    )(*arrived)


def solution(mesh):
    in_specs = (
        P(("groups", "pages"), "heads"),
        P(("groups", "pages"), "heads"),
        P(("groups", "pages"), None),
        P("heads", None, None),
        P("heads", None, None),
        P("groups"),
        P("groups"),
        P("groups"),
    )
    body = functools.partial(on_device, members=mesh.shape["pages"], devices=mesh.shape["heads"])
    return jax.shard_map(
        body, mesh=mesh, in_specs=in_specs, out_specs=P(("groups", "pages"), "heads"), check_vma=False
    )
```

```python
import functools

import jax
import jax.numpy as jnp
from jax import lax
from jax.experimental import pallas as pl
from jax.experimental.pallas import tpu as pltpu
from jax.sharding import PartitionSpec as P


PAGE = 64
GROUP = 2
LANES = 4
BLOCK_PAGES = 8
HEADS_STEP = 8
PIECES = 2
CHUNKS = 1


FLOOR = -1e30
FAR = 2**30
LOG2E = 1.4426950408889634


def pack_kernel(dims, nope_ref, rope_ref, cache_ref, *refs):
    nope_width, rope_width, quarter_cols, chunks = dims
    outs, sems = refs[:-1], refs[-1]
    mine = lax.axis_index("pages") % GROUP
    lane = lax.axis_index("heads") % LANES
    depth = cache_ref.shape[0] // PIECES
    copies = []
    for p in range(PIECES):
        copies.append(
            pltpu.make_async_copy(
                cache_ref.at[pl.ds(p * depth, depth), pl.ds(pl.multiple_of(lane * quarter_cols, 128), quarter_cols)],
                outs[p],
                sems.at[p],
            )
        )
    for c in range(chunks):
        for e in range(GROUP):
            which = ((mine + e) % GROUP) * chunks + c
            for ref, width, at in ((nope_ref, nope_width, 0), (rope_ref, rope_width, nope_width)):
                copies.append(
                    pltpu.make_async_copy(
                        ref.at[:, pl.ds(pl.multiple_of(which * width, 128), width)],
                        outs[PIECES + c * GROUP + e].at[:, pl.ds(at, width)],
                        sems.at[len(copies)],
                    )
                )
    for c in copies:
        c.start()
    for c in copies:
        c.wait()


def absorb_kernel(dims, tok_ref, off_ref, *refs):
    members, first, hc, hh, nope, rope, latent = dims
    q_refs, keys_hbm, qs_ref, limit_ref, wk, turned, sem = refs[:members], *refs[members:]
    rows = limit_ref.shape[0]
    local_rows = rows // members
    member = lax.axis_index("pages")
    mine = member % GROUP
    copy = pltpu.make_async_copy(keys_hbm.at[pl.ds(mine * hh + first, hc)], wk, sem)
    copy.start()
    token = pltpu.roll(
        jnp.broadcast_to(tok_ref[...], (8, rows)), lax.rem(rows - member * local_rows, rows), axis=1
    )[:1]
    across = lax.broadcasted_iota(jnp.int32, (rows, rows), 1)
    down = lax.broadcasted_iota(jnp.int32, (rows, rows), 0)
    wanted = lax.rem(member - down // local_rows + members, members) * local_rows + lax.rem(down, local_rows)
    order = (jnp.broadcast_to(token, (rows, rows)) == wanted).astype(jnp.bfloat16)
    limit = jnp.max(jnp.where(across == wanted, off_ref[...], 0), axis=1, keepdims=True)
    limit_ref[...] = jnp.broadcast_to(limit, limit_ref.shape)
    whole = jnp.concatenate([q[...] for q in q_refs], axis=0)
    turned[...] = jnp.dot(order, whole, preferred_element_type=jnp.float32).astype(jnp.bfloat16)
    copy.wait()
    for h in range(hc):
        lat = jnp.dot(turned[:, h * nope:(h + 1) * nope], wk[h], preferred_element_type=jnp.float32)
        qs_ref[h * rows:(h + 1) * rows, :latent] = lat.astype(jnp.bfloat16)
        at = hc * nope + h * rope
        qs_ref[h * rows:(h + 1) * rows, latent:] = turned[:, at:at + rope]


def attend_kernel(dims, counts_ref, limit_ref, qs_hbm, *refs):
    members, first, hc, hh, hb, nope, rope, latent, vhead, rows, slots = dims
    part_refs, refs = refs[:LANES * PIECES], refs[LANES * PIECES:]
    own_ref, values_hbm = refs[:2]
    out_refs, refs = refs[2:2 + members], refs[2 + members:]
    tiles, wv, bias, qs, sbuf, mx, den, acc, lse, sems, own_sems, part_sems = refs
    local_rows = rows // members
    block = BLOCK_PAGES * PAGE
    cols = slots * PAGE
    quarter_cols = cols // LANES
    depth = (latent + rope) // PIECES
    scale2 = (nope + rope) ** (-0.5) * LOG2E
    steps = hc // hb
    group_rows = hb * rows
    member = lax.axis_index("pages")
    lane_id = lax.axis_index("heads") % LANES
    partner = member ^ 1
    mine = member % GROUP
    own_live, part_live = counts_ref[member], counts_ref[partner]
    own_blocks = (own_live + BLOCK_PAGES - 1) // BLOCK_PAGES
    part_blocks = (part_live + BLOCK_PAGES - 1) // BLOCK_PAGES
    blocks = own_blocks + part_blocks

    query_copies = [
        pltpu.make_async_copy(
            qs_hbm.at[pl.ds(g * group_rows, group_rows)], qs.at[pl.ds(g * group_rows, group_rows)], sems.at[g]
        )
        for g in range(steps)
    ]
    value_copy = pltpu.make_async_copy(values_hbm.at[pl.ds(mine * hh + first, hc)], wv, sems.at[steps])
    tile_copies = []
    for b in range(-(-cols // block)):
        at = pl.ds(b * block, min(block, cols - b * block))
        tile_copies.append((b < own_blocks, pltpu.make_async_copy(own_ref.at[:, at], tiles.at[:, at], own_sems.at[b])))
    for i, flip in enumerate((0, 2, 1, 3)):
        quarter = lane_id ^ flip
        at = pl.multiple_of(cols + quarter * quarter_cols, 128)
        for p in range(PIECES):
            tile_copies.append((
                quarter * quarter_cols < part_blocks * block,
                pltpu.make_async_copy(
                    part_refs[i * PIECES + p],
                    tiles.at[pl.ds(p * depth, depth), pl.ds(at, quarter_cols)],
                    part_sems.at[i * PIECES + p],
                ),
            ))
    query_copies[0].start()
    for used, copy in tile_copies:
        pl.when(used)(copy.start)
    for copy in query_copies[1:] + [value_copy]:
        copy.start()

    before = lambda who: lax.fori_loop(0, who, lambda i, total: total + counts_ref[i], jnp.int32(0))
    limit = limit_ref[:, :1]
    own_base, part_base = before(member) * PAGE, before(partner) * PAGE

    def column(b):
        return pl.multiple_of(jnp.where(b < own_blocks, b * block, cols + (b - own_blocks) * block), 128)

    spot = lax.broadcasted_iota(jnp.int32, (1, block), 1)

    def fill_bias(b, carry):
        own = b < own_blocks
        inside = jnp.where(own, b, b - own_blocks) * block + spot
        live = jnp.where(own, own_live, part_live) * PAGE
        positions = jnp.where(inside < live, jnp.where(own, own_base, part_base) + inside, FAR)
        bias[:, pl.ds(pl.multiple_of(b * block, 128), block)] = jnp.where(positions < limit, 0.0, FLOOR)
        return carry

    lax.fori_loop(0, blocks, fill_bias, 0)
    lse[...] = jnp.zeros_like(lse)

    def score(g, b):
        slot = g % 2
        scores = jnp.dot(qs[g * group_rows:(g + 1) * group_rows], tiles[:, pl.ds(column(b), block)], preferred_element_type=jnp.float32)
        at = pl.multiple_of(b * block, 128)
        shut = bias[:, pl.ds(at, block)]
        for e in range(hb):
            part = slice(e * rows, (e + 1) * rows)
            value = scores[part] + shut
            sbuf[slot, part, pl.ds(at, block)] = value
            top = functools.reduce(jnp.maximum, [value[:, i:i + 128] for i in range(0, block, 128)])
            mx[slot, part] = jnp.maximum(mx[slot, part], top)

    def gather(g, b, top):
        slot = g % 2
        at = pl.multiple_of(b * block, 128)
        weights = jnp.exp2((sbuf[slot, :, pl.ds(at, block)] - top) * scale2)
        den[...] += functools.reduce(jnp.add, [weights[:, i:i + 128] for i in range(0, block, 128)])
        acc[...] += lax.dot_general(
            weights.astype(jnp.bfloat16),
            tiles[:latent, pl.ds(column(b), block)],
            (((1,), (1,)), ((), ())),
            preferred_element_type=jnp.float32,
        )

    lane = lax.broadcasted_iota(jnp.int32, (rows, 128), 1)

    def finish(g, top):
        total = jnp.sum(den[...], axis=1, keepdims=True)
        seen = top > 0.5 * FLOOR
        total = jnp.where(seen, total, 1.0)
        share = jnp.where(seen, 1.0 / total, 0.0)
        logs = jnp.where(seen, top * scale2 + jnp.log2(total), FLOOR)
        for e in range(hb):
            h = g * hb + e
            part = slice(e * rows, (e + 1) * rows)
            value = jnp.dot(acc[part].astype(jnp.bfloat16), wv[h], preferred_element_type=jnp.float32)
            value = (value * share[part]).astype(jnp.bfloat16)
            for s in range(members):
                out_refs[s][:, h * vhead:(h + 1) * vhead] = value[s * local_rows:(s + 1) * local_rows]
            full = logs[part]
            high = full.astype(jnp.bfloat16).astype(jnp.float32)
            middle = (full - high).astype(jnp.bfloat16).astype(jnp.float32)
            low = full - high - middle
            lse[...] = jnp.where(lane == h, high, jnp.where(lane == hc + h, middle,
                                 jnp.where(lane == 2 * hc + h, low, lse[...])))

    top = None
    for g in range(steps + 1):
        if g < steps:
            query_copies[g].wait()
            mx[g % 2] = jnp.full(mx.shape[1:], FLOOR, jnp.float32)
        if g == 0:
            for used, copy in tile_copies:
                pl.when(used)(copy.wait)
        if g == 1:
            value_copy.wait()
        if g > 0:
            den[...] = jnp.zeros_like(den)
            acc[...] = jnp.zeros_like(acc)

        def body(b, carry, g=g, top=top):
            if g < steps:
                score(g, b)
            if g > 0:
                gather(g - 1, b, top)
            return carry

        lax.fori_loop(0, blocks, body, 0)
        if g > 0:
            finish(g - 1, top)
        if g < steps:
            top = jnp.max(mx[g % 2], axis=1, keepdims=True)

    for s in range(members):
        out_refs[s][:, hc * vhead:] = lse[s * local_rows:(s + 1) * local_rows].astype(jnp.bfloat16)


def attend_call(members, first, hc, hh, hb, nope, rope, latent, vhead, rows, slots, chunks):
    hbm = pl.BlockSpec(memory_space=pltpu.HBM)
    vmem = pl.BlockSpec(memory_space=pltpu.VMEM)
    bf16 = jnp.bfloat16
    full = latent + rope
    cols = slots * PAGE
    local_rows = rows // members
    packed = hc * vhead + 128
    block = BLOCK_PAGES * PAGE
    most = 2 * (-(-cols // block))
    return pl.pallas_call(
        functools.partial(
            attend_kernel, (members, first, hc, hh, hb, nope, rope, latent, vhead, rows, slots)
        ),
        out_shape=[jax.ShapeDtypeStruct((local_rows, packed), bf16)] * members,
        in_specs=[pl.BlockSpec(memory_space=pltpu.SMEM), vmem] + [hbm] * (1 + LANES * PIECES + 2),
        out_specs=[vmem] * members,
        scratch_shapes=[
            pltpu.VMEM((full, 2 * cols), bf16),
            pltpu.VMEM((hc, latent, vhead), bf16),
            pltpu.VMEM((rows, most * block), jnp.float32),
            pltpu.VMEM((hc * rows, full), bf16),
            pltpu.VMEM((2, hb * rows, most * block), jnp.float32),
            pltpu.VMEM((2, hb * rows, 128), jnp.float32),
            pltpu.VMEM((hb * rows, 128), jnp.float32),
            pltpu.VMEM((hb * rows, latent), jnp.float32),
            pltpu.VMEM((rows, 128), jnp.float32),
            pltpu.SemaphoreType.DMA((1 + hc // hb,)),
            pltpu.SemaphoreType.DMA((most // 2,)),
            pltpu.SemaphoreType.DMA((LANES * PIECES,)),
        ],
        compiler_params=pltpu.CompilerParams(vmem_limit_bytes=56 << 20),
        cost_estimate=pl.CostEstimate(flops=8 * 10**9 // chunks, bytes_accessed=8 * 10**6, transcendentals=0),
    )


def merge_kernel(dims, *refs):
    hc, vhead, members, chunks = dims
    out_ref = refs[-1]
    mine = lax.axis_index("pages") % GROUP
    for c in range(chunks):
        for parity in range(GROUP):
            parts = [refs[c * members + s] for s in range(members) if s % GROUP == parity]
            logs = []
            for b in parts:
                packed = b[:, hc * vhead:].astype(jnp.float32)
                logs.append(packed[:, :hc] + packed[:, hc:2 * hc] + packed[:, 2 * hc:3 * hc])
            top = functools.reduce(jnp.maximum, logs)
            weights = [jnp.exp2(v - top) for v in logs]
            total = functools.reduce(jnp.add, weights)
            weights = [w / total for w in weights]
            base = (lax.rem(mine + parity, GROUP) * chunks + c) * (hc * vhead)
            for h in range(hc):
                cols = slice(h * vhead, (h + 1) * vhead)
                value = functools.reduce(
                    jnp.add, [w[:, h:h + 1] * b[:, cols].astype(jnp.float32) for w, b in zip(weights, parts)]
                )
                out_ref[:, pl.ds(pl.multiple_of(base + h * vhead, 128), vhead)] = value.astype(jnp.bfloat16)


def on_device(
    q_nope, q_rope, cache_tiles, absorb_keys, absorb_values, page_counts, query_token, query_offsets, members, devices
):
    heads_here, nope, latent = absorb_keys.shape
    vhead = absorb_values.shape[2]
    local_rows = q_nope.shape[0]
    rope = q_rope.shape[1] // heads_here
    full = cache_tiles.shape[1]
    slots = cache_tiles.shape[0] // PAGE
    cols = slots * PAGE
    rows = local_rows * members
    hh = heads_here // GROUP
    chunks = min(CHUNKS, hh // 2)
    hc = hh // chunks
    hb = min(HEADS_STEP, hc)
    hbm = pl.BlockSpec(memory_space=pltpu.HBM)
    vmem = pl.BlockSpec(memory_space=pltpu.VMEM)
    bf16 = jnp.bfloat16

    def over_pages(x, s):
        return lax.ppermute(x, "pages", [(i, (i - s) % members) for i in range(members)])

    def over_heads(x, bit):
        return lax.ppermute(x, "heads", [(i, i ^ bit) for i in range(devices)])

    turned = cache_tiles.T
    packed = pl.pallas_call(
        functools.partial(pack_kernel, (hc * nope, hc * rope, cols // LANES, chunks)),
        out_shape=[jax.ShapeDtypeStruct((full // PIECES, cols // LANES), bf16)] * PIECES
        + [jax.ShapeDtypeStruct((local_rows, hc * (nope + rope)), bf16)] * (GROUP * chunks),
        in_specs=[hbm] * 3,
        out_specs=[vmem] * (PIECES + GROUP * chunks),
        scratch_shapes=[pltpu.SemaphoreType.DMA((PIECES + 2 * GROUP * chunks,))],
        name="pack",
    )(q_nope, q_rope, turned)
    pieces, shares = packed[:PIECES], packed[PIECES:]

    parts = [[None] * PIECES for _ in range(LANES)]
    for p in range(PIECES):
        parts[0][p] = lax.ppermute(pieces[p], "pages", [(i, i ^ 1) for i in range(members)])
        parts[1][p] = over_heads(parts[0][p], 2)
        parts[2][p] = over_heads(parts[0][p], 1)
        parts[3][p] = over_heads(parts[1][p], 1)
    parts = [p for part in parts for p in part]
    absorbed = []
    for c in range(chunks):
        own, other = shares[c * GROUP:(c + 1) * GROUP]
        blocks = [own]
        for s in range(1, members):
            blocks.append(over_pages((own, other)[s % GROUP], s))
        absorbed.append(pl.pallas_call(
            functools.partial(absorb_kernel, (members, c * hc, hc, hh, nope, rope, latent)),
            out_shape=[
                jax.ShapeDtypeStruct((hc * rows, full), bf16),
                jax.ShapeDtypeStruct((rows, 128), jnp.int32),
            ],
            in_specs=[vmem] * (2 + members) + [hbm],
            out_specs=[vmem] * 2,
            scratch_shapes=[
                pltpu.VMEM((hc, nope, latent), bf16),
                pltpu.VMEM((rows, hc * (nope + rope)), bf16),
                pltpu.SemaphoreType.DMA(()),
            ],
        )(query_token[None, :], query_offsets[None, :], *blocks, absorb_keys))

    arrived = []
    for c in range(chunks):
        outs = attend_call(
            members, c * hc, hc, hh, hb, nope, rope, latent, vhead, rows, slots, chunks
        )(page_counts, absorbed[c][1], absorbed[c][0], *parts, turned, absorb_values)
        arrived.append(outs[0])
        for s in range(1, members):
            arrived.append(over_pages(outs[s], s))

    return pl.pallas_call(
        functools.partial(merge_kernel, (hc, vhead, members, chunks)),
        out_shape=jax.ShapeDtypeStruct((local_rows, heads_here * vhead), bf16),
        in_specs=[vmem] * (members * chunks),
        out_specs=vmem,
        name="merge",
    )(*arrived)


def solution(mesh):
    in_specs = (
        P(("groups", "pages"), "heads"),
        P(("groups", "pages"), "heads"),
        P(("groups", "pages"), None),
        P("heads", None, None),
        P("heads", None, None),
        P("groups"),
        P("groups"),
        P("groups"),
    )
    body = functools.partial(on_device, members=mesh.shape["pages"], devices=mesh.shape["heads"])
    return jax.shard_map(
        body, mesh=mesh, in_specs=in_specs, out_specs=P(("groups", "pages"), "heads"), check_vma=False
    )
```

```python
import functools

import jax
import jax.numpy as jnp
from jax import lax
from jax.experimental import pallas as pl
from jax.experimental.pallas import tpu as pltpu
from jax.sharding import PartitionSpec as P


PAGE = 64
GROUP = 2
LANES = 4
BLOCK_PAGES = 8
HEADS_STEP = 8
PIECES = 2
CHUNKS = 1


FLOOR = -1e30
FAR = 2**30
LOG2E = 1.4426950408889634


def pack_pages_kernel(quarter_cols, cache_ref, *refs):
    outs, sems = refs[:-1], refs[-1]
    lane = lax.axis_index("heads") % LANES
    depth = cache_ref.shape[0] // PIECES
    at = pl.ds(pl.multiple_of(lane * quarter_cols, 128), quarter_cols)
    copies = [
        pltpu.make_async_copy(cache_ref.at[pl.ds(p * depth, depth), at], outs[p], sems.at[p]) for p in range(PIECES)
    ]
    for c in copies:
        c.start()
    for c in copies:
        c.wait()


def pack_queries_kernel(dims, nope_ref, rope_ref, *refs):
    nope_width, rope_width, chunks = dims
    outs, sems = refs[:-1], refs[-1]
    mine = lax.axis_index("pages") % GROUP
    copies = []
    for c in range(chunks):
        for e in range(GROUP):
            which = ((mine + e) % GROUP) * chunks + c
            for ref, width, at in ((nope_ref, nope_width, 0), (rope_ref, rope_width, nope_width)):
                copies.append(
                    pltpu.make_async_copy(
                        ref.at[:, pl.ds(pl.multiple_of(which * width, 128), width)],
                        outs[c * GROUP + e].at[:, pl.ds(at, width)],
                        sems.at[len(copies)],
                    )
                )
    for c in copies:
        c.start()
    for c in copies:
        c.wait()


def attend_kernel(dims, counts_ref, tok_ref, off_ref, *refs):
    members, first, hc, hh, hb, nope, rope, latent, vhead, rows, slots = dims
    q_refs, refs = refs[:members], refs[members:]
    part_refs, refs = refs[:LANES * PIECES], refs[LANES * PIECES:]
    own_ref, keys_hbm, values_hbm = refs[:3]
    out_refs, refs = refs[3:3 + members], refs[3 + members:]
    raw, turned, wk, wv, tiles, bias, qs, sbuf, mx, den, acc, lse, sems, own_sems, part_sems = refs
    local_rows = rows // members
    block = BLOCK_PAGES * PAGE
    cols = slots * PAGE
    quarter_cols = cols // LANES
    depth = (latent + rope) // PIECES
    scale2 = (nope + rope) ** (-0.5) * LOG2E
    steps = hc // hb
    group_rows = hb * rows
    member = lax.axis_index("pages")
    lane_id = lax.axis_index("heads") % LANES
    partner = member ^ 1
    mine = member % GROUP
    own_live, part_live = counts_ref[member], counts_ref[partner]
    own_blocks = (own_live + BLOCK_PAGES - 1) // BLOCK_PAGES
    part_blocks = (part_live + BLOCK_PAGES - 1) // BLOCK_PAGES
    blocks = own_blocks + part_blocks

    query_copies = [
        pltpu.make_async_copy(q, raw.at[pl.ds(s * local_rows, local_rows)], sems.at[2 + s])
        for s, q in enumerate(q_refs)
    ]
    key_copy = pltpu.make_async_copy(keys_hbm.at[pl.ds(mine * hh + first, hc)], wk, sems.at[0])
    value_copy = pltpu.make_async_copy(values_hbm.at[pl.ds(mine * hh + first, hc)], wv, sems.at[1])
    tile_copies = []
    for b in range(-(-cols // block)):
        at = pl.ds(b * block, min(block, cols - b * block))
        tile_copies.append((b < own_blocks, pltpu.make_async_copy(own_ref.at[:, at], tiles.at[:, at], own_sems.at[b])))
    for i, flip in enumerate((0, 2, 1, 3)):
        quarter = lane_id ^ flip
        at = pl.multiple_of(cols + quarter * quarter_cols, 128)
        for p in range(PIECES):
            tile_copies.append((
                quarter * quarter_cols < part_blocks * block,
                pltpu.make_async_copy(
                    part_refs[i * PIECES + p],
                    tiles.at[pl.ds(p * depth, depth), pl.ds(at, quarter_cols)],
                    part_sems.at[i * PIECES + p],
                ),
            ))
    for copy in query_copies + [key_copy]:
        copy.start()
    for used, copy in tile_copies:
        pl.when(used)(copy.start)
    value_copy.start()

    token = pltpu.roll(
        jnp.broadcast_to(tok_ref[...], (8, rows)), lax.rem(rows - member * local_rows, rows), axis=1
    )[:1]
    across = lax.broadcasted_iota(jnp.int32, (rows, rows), 1)
    down = lax.broadcasted_iota(jnp.int32, (rows, rows), 0)
    wanted = lax.rem(member - down // local_rows + members, members) * local_rows + lax.rem(down, local_rows)
    order = (jnp.broadcast_to(token, (rows, rows)) == wanted).astype(jnp.bfloat16)
    limit = jnp.max(jnp.where(across == wanted, off_ref[...], 0), axis=1, keepdims=True)

    before = lambda who: lax.fori_loop(0, who, lambda i, total: total + counts_ref[i], jnp.int32(0))
    own_base, part_base = before(member) * PAGE, before(partner) * PAGE

    def column(b):
        return pl.multiple_of(jnp.where(b < own_blocks, b * block, cols + (b - own_blocks) * block), 128)

    spot = lax.broadcasted_iota(jnp.int32, (1, block), 1)

    def fill_bias(b, carry):
        own = b < own_blocks
        inside = jnp.where(own, b, b - own_blocks) * block + spot
        live = jnp.where(own, own_live, part_live) * PAGE
        positions = jnp.where(inside < live, jnp.where(own, own_base, part_base) + inside, FAR)
        bias[:, pl.ds(pl.multiple_of(b * block, 128), block)] = jnp.where(positions < limit, 0.0, FLOOR)
        return carry

    lax.fori_loop(0, blocks, fill_bias, 0)
    lse[...] = jnp.zeros_like(lse)

    for copy in query_copies:
        copy.wait()
    turned[...] = jnp.dot(order, raw[...], preferred_element_type=jnp.float32).astype(jnp.bfloat16)
    key_copy.wait()

    def absorb(g):
        for h in range(g * hb, (g + 1) * hb):
            lat = jnp.dot(turned[:, h * nope:(h + 1) * nope], wk[h], preferred_element_type=jnp.float32)
            qs[h * rows:(h + 1) * rows, :latent] = lat.astype(jnp.bfloat16)
            at = hc * nope + h * rope
            qs[h * rows:(h + 1) * rows, latent:] = turned[:, at:at + rope]

    def score(g, b):
        slot = g % 2
        scores = jnp.dot(qs[g * group_rows:(g + 1) * group_rows], tiles[:, pl.ds(column(b), block)], preferred_element_type=jnp.float32)
        at = pl.multiple_of(b * block, 128)
        shut = bias[:, pl.ds(at, block)]
        for e in range(hb):
            part = slice(e * rows, (e + 1) * rows)
            value = scores[part] + shut
            sbuf[slot, part, pl.ds(at, block)] = value
            top = functools.reduce(jnp.maximum, [value[:, i:i + 128] for i in range(0, block, 128)])
            mx[slot, part] = jnp.maximum(mx[slot, part], top)

    def gather(g, b, top):
        slot = g % 2
        at = pl.multiple_of(b * block, 128)
        weights = jnp.exp2((sbuf[slot, :, pl.ds(at, block)] - top) * scale2)
        den[...] += functools.reduce(jnp.add, [weights[:, i:i + 128] for i in range(0, block, 128)])
        acc[...] += lax.dot_general(
            weights.astype(jnp.bfloat16),
            tiles[:latent, pl.ds(column(b), block)],
            (((1,), (1,)), ((), ())),
            preferred_element_type=jnp.float32,
        )

    lane = lax.broadcasted_iota(jnp.int32, (rows, 128), 1)

    def finish(g, top):
        total = jnp.sum(den[...], axis=1, keepdims=True)
        seen = top > 0.5 * FLOOR
        total = jnp.where(seen, total, 1.0)
        share = jnp.where(seen, 1.0 / total, 0.0)
        logs = jnp.where(seen, top * scale2 + jnp.log2(total), FLOOR)
        for e in range(hb):
            h = g * hb + e
            part = slice(e * rows, (e + 1) * rows)
            value = jnp.dot(acc[part].astype(jnp.bfloat16), wv[h], preferred_element_type=jnp.float32)
            value = (value * share[part]).astype(jnp.bfloat16)
            for s in range(members):
                out_refs[s][:, h * vhead:(h + 1) * vhead] = value[s * local_rows:(s + 1) * local_rows]
            full = logs[part]
            high = full.astype(jnp.bfloat16).astype(jnp.float32)
            middle = (full - high).astype(jnp.bfloat16).astype(jnp.float32)
            low = full - high - middle
            lse[...] = jnp.where(lane == h, high, jnp.where(lane == hc + h, middle,
                                 jnp.where(lane == 2 * hc + h, low, lse[...])))

    top = None
    for g in range(steps + 1):
        if g < steps:
            absorb(g)
            mx[g % 2] = jnp.full(mx.shape[1:], FLOOR, jnp.float32)
        if g == 0:
            for used, copy in tile_copies:
                pl.when(used)(copy.wait)
        if g == 1:
            value_copy.wait()
        if g > 0:
            den[...] = jnp.zeros_like(den)
            acc[...] = jnp.zeros_like(acc)

        def body(b, carry, g=g, top=top):
            if g < steps:
                score(g, b)
            if g > 0:
                gather(g - 1, b, top)
            return carry

        lax.fori_loop(0, blocks, body, 0)
        if g > 0:
            finish(g - 1, top)
        if g < steps:
            top = jnp.max(mx[g % 2], axis=1, keepdims=True)

    for s in range(members):
        out_refs[s][:, hc * vhead:] = lse[s * local_rows:(s + 1) * local_rows].astype(jnp.bfloat16)


def attend_call(members, first, hc, hh, hb, nope, rope, latent, vhead, rows, slots, chunks):
    hbm = pl.BlockSpec(memory_space=pltpu.HBM)
    vmem = pl.BlockSpec(memory_space=pltpu.VMEM)
    bf16 = jnp.bfloat16
    full = latent + rope
    cols = slots * PAGE
    local_rows = rows // members
    packed = hc * vhead + 128
    block = BLOCK_PAGES * PAGE
    most = 2 * (-(-cols // block))
    return pl.pallas_call(
        functools.partial(
            attend_kernel, (members, first, hc, hh, hb, nope, rope, latent, vhead, rows, slots)
        ),
        out_shape=[jax.ShapeDtypeStruct((local_rows, packed), bf16)] * members,
        in_specs=[pl.BlockSpec(memory_space=pltpu.SMEM), vmem, vmem] + [hbm] * (members + LANES * PIECES + 3),
        out_specs=[vmem] * members,
        scratch_shapes=[
            pltpu.VMEM((rows, hc * (nope + rope)), bf16),
            pltpu.VMEM((rows, hc * (nope + rope)), bf16),
            pltpu.VMEM((hc, nope, latent), bf16),
            pltpu.VMEM((hc, latent, vhead), bf16),
            pltpu.VMEM((full, 2 * cols), bf16),
            pltpu.VMEM((rows, most * block), jnp.float32),
            pltpu.VMEM((hc * rows, full), bf16),
            pltpu.VMEM((2, hb * rows, most * block), jnp.float32),
            pltpu.VMEM((2, hb * rows, 128), jnp.float32),
            pltpu.VMEM((hb * rows, 128), jnp.float32),
            pltpu.VMEM((hb * rows, latent), jnp.float32),
            pltpu.VMEM((rows, 128), jnp.float32),
            pltpu.SemaphoreType.DMA((2 + members,)),
            pltpu.SemaphoreType.DMA((most // 2,)),
            pltpu.SemaphoreType.DMA((LANES * PIECES,)),
        ],
        compiler_params=pltpu.CompilerParams(vmem_limit_bytes=56 << 20),
        cost_estimate=pl.CostEstimate(flops=8 * 10**9 // chunks, bytes_accessed=8 * 10**6, transcendentals=0),
    )


def merge_kernel(dims, *refs):
    hc, vhead, members, chunks = dims
    out_ref = refs[-1]
    mine = lax.axis_index("pages") % GROUP
    for c in range(chunks):
        for parity in range(GROUP):
            parts = [refs[c * members + s] for s in range(members) if s % GROUP == parity]
            logs = []
            for b in parts:
                packed = b[:, hc * vhead:].astype(jnp.float32)
                logs.append(packed[:, :hc] + packed[:, hc:2 * hc] + packed[:, 2 * hc:3 * hc])
            top = functools.reduce(jnp.maximum, logs)
            weights = [jnp.exp2(v - top) for v in logs]
            total = functools.reduce(jnp.add, weights)
            weights = [w / total for w in weights]
            base = (lax.rem(mine + parity, GROUP) * chunks + c) * (hc * vhead)
            for h in range(hc):
                cols = slice(h * vhead, (h + 1) * vhead)
                value = functools.reduce(
                    jnp.add, [w[:, h:h + 1] * b[:, cols].astype(jnp.float32) for w, b in zip(weights, parts)]
                )
                out_ref[:, pl.ds(pl.multiple_of(base + h * vhead, 128), vhead)] = value.astype(jnp.bfloat16)


def on_device(
    q_nope, q_rope, cache_tiles, absorb_keys, absorb_values, page_counts, query_token, query_offsets, members, devices
):
    heads_here, nope, latent = absorb_keys.shape
    vhead = absorb_values.shape[2]
    local_rows = q_nope.shape[0]
    rope = q_rope.shape[1] // heads_here
    full = cache_tiles.shape[1]
    slots = cache_tiles.shape[0] // PAGE
    cols = slots * PAGE
    rows = local_rows * members
    hh = heads_here // GROUP
    chunks = min(CHUNKS, hh // 2)
    hc = hh // chunks
    hb = min(HEADS_STEP, hc)
    hbm = pl.BlockSpec(memory_space=pltpu.HBM)
    vmem = pl.BlockSpec(memory_space=pltpu.VMEM)
    bf16 = jnp.bfloat16

    def over_pages(x, s):
        return lax.ppermute(x, "pages", [(i, (i - s) % members) for i in range(members)])

    def over_heads(x, bit):
        return lax.ppermute(x, "heads", [(i, i ^ bit) for i in range(devices)])

    turned = cache_tiles.T
    pieces = pl.pallas_call(
        functools.partial(pack_pages_kernel, cols // LANES),
        out_shape=[jax.ShapeDtypeStruct((full // PIECES, cols // LANES), bf16)] * PIECES,
        in_specs=[hbm],
        out_specs=[vmem] * PIECES,
        scratch_shapes=[pltpu.SemaphoreType.DMA((PIECES,))],
        name="pack_pages",
    )(turned)
    shares = pl.pallas_call(
        functools.partial(pack_queries_kernel, (hc * nope, hc * rope, chunks)),
        out_shape=[jax.ShapeDtypeStruct((local_rows, hc * (nope + rope)), bf16)] * (GROUP * chunks),
        in_specs=[hbm] * 2,
        out_specs=[vmem] * (GROUP * chunks),
        scratch_shapes=[pltpu.SemaphoreType.DMA((2 * GROUP * chunks,))],
        name="pack_queries",
    )(q_nope, q_rope)

    parts = [[None] * PIECES for _ in range(LANES)]
    for p in range(PIECES):
        parts[0][p] = lax.ppermute(pieces[p], "pages", [(i, i ^ 1) for i in range(members)])
        parts[1][p] = over_heads(parts[0][p], 2)
        parts[2][p] = over_heads(parts[0][p], 1)
        parts[3][p] = over_heads(parts[1][p], 1)
    parts = [p for part in parts for p in part]
    queries = []
    for c in range(chunks):
        own, other = shares[c * GROUP:(c + 1) * GROUP]
        blocks = [own]
        for s in range(1, members):
            blocks.append(over_pages((own, other)[s % GROUP], s))
        queries.append(blocks)

    arrived = []
    for c in range(chunks):
        outs = attend_call(
            members, c * hc, hc, hh, hb, nope, rope, latent, vhead, rows, slots, chunks
        )(page_counts, query_token[None, :], query_offsets[None, :], *queries[c], *parts, turned, absorb_keys,
          absorb_values)
        arrived.append(outs[0])
        for s in range(1, members):
            arrived.append(over_pages(outs[s], s))

    return pl.pallas_call(
        functools.partial(merge_kernel, (hc, vhead, members, chunks)),
        out_shape=jax.ShapeDtypeStruct((local_rows, heads_here * vhead), bf16),
        in_specs=[vmem] * (members * chunks),
        out_specs=vmem,
        name="merge",
    )(*arrived)


def solution(mesh):
    in_specs = (
        P(("groups", "pages"), "heads"),
        P(("groups", "pages"), "heads"),
        P(("groups", "pages"), None),
        P("heads", None, None),
        P("heads", None, None),
        P("groups"),
        P("groups"),
        P("groups"),
    )
    body = functools.partial(on_device, members=mesh.shape["pages"], devices=mesh.shape["heads"])
    return jax.shard_map(
        body, mesh=mesh, in_specs=in_specs, out_specs=P(("groups", "pages"), "heads"), check_vma=False
    )
```

```python
import functools

import jax
import jax.numpy as jnp
from jax import lax
from jax.experimental import pallas as pl
from jax.experimental.pallas import tpu as pltpu
from jax.sharding import PartitionSpec as P


PAGE = 64
GROUP = 2
LANES = 4
BLOCK_PAGES = 4
PIECES = 2
HALVES = 2


FLOOR = -1e30
FAR = 2**30
LOG2E = 1.4426950408889634


def pack_pages_kernel(quarter_cols, cache_ref, *refs):
    outs, sems = refs[:-1], refs[-1]
    lane = lax.axis_index("heads") % LANES
    depth = cache_ref.shape[0] // PIECES
    at = pl.ds(pl.multiple_of(lane * quarter_cols, 128), quarter_cols)
    copies = [
        pltpu.make_async_copy(cache_ref.at[pl.ds(p * depth, depth), at], outs[p], sems.at[p]) for p in range(PIECES)
    ]
    for c in copies:
        c.start()
    for c in copies:
        c.wait()


def pack_queries_kernel(dims, nope_ref, rope_ref, *refs):
    nope_width, rope_width = dims
    outs, sems = refs[:-1], refs[-1]
    mine = lax.axis_index("pages") % GROUP
    copies = []
    for e in range(GROUP):
        which = (mine + e) % GROUP
        for ref, width, at in ((nope_ref, nope_width, 0), (rope_ref, rope_width, nope_width)):
            copies.append(
                pltpu.make_async_copy(
                    ref.at[:, pl.ds(pl.multiple_of(which * width, 128), width)],
                    outs[e].at[:, pl.ds(at, width)],
                    sems.at[len(copies)],
                )
            )
    for c in copies:
        c.start()
    for c in copies:
        c.wait()


def attend_kernel(dims, counts_ref, tok_ref, off_ref, *refs):
    members, hh, nope, rope, latent, vhead, rows, slots = dims
    q_refs, refs = refs[:members], refs[members:]
    part_refs, refs = refs[:LANES * PIECES], refs[LANES * PIECES:]
    own_ref, keys_hbm, values_hbm = refs[:3]
    out_refs, refs = refs[3:3 + members], refs[3 + members:]
    raw, turned, wk, wv, tiles, bias, qs, sbuf, mx, den, acc, sums, flat, sems, own_sems, part_sems = refs
    local_rows = rows // members
    block = BLOCK_PAGES * PAGE
    cols = slots * PAGE
    quarter_cols = cols // LANES
    depth = (latent + rope) // PIECES
    scale2 = (nope + rope) ** (-0.5) * LOG2E
    half = rows // HALVES
    group_rows = hh * half
    member = lax.axis_index("pages")
    lane_id = lax.axis_index("heads") % LANES
    partner = member ^ 1
    mine = member % GROUP
    own_live, part_live = counts_ref[member], counts_ref[partner]
    own_blocks = (own_live + BLOCK_PAGES - 1) // BLOCK_PAGES
    part_blocks = (part_live + BLOCK_PAGES - 1) // BLOCK_PAGES

    query_copies = [
        pltpu.make_async_copy(q, raw.at[pl.ds(s * local_rows, local_rows)], sems.at[2 + s])
        for s, q in enumerate(q_refs)
    ]
    key_copy = pltpu.make_async_copy(keys_hbm.at[pl.ds(mine * hh, hh)], wk, sems.at[0])
    value_copy = pltpu.make_async_copy(values_hbm.at[pl.ds(mine * hh, hh)], wv, sems.at[1])
    tile_copies = []
    for b in range(-(-cols // block)):
        at = pl.ds(b * block, min(block, cols - b * block))
        tile_copies.append((b < own_blocks, pltpu.make_async_copy(own_ref.at[:, at], tiles.at[:, at], own_sems.at[b])))
    for i, flip in enumerate((0, 2, 1, 3)):
        quarter = lane_id ^ flip
        at = pl.multiple_of(cols + quarter * quarter_cols, 128)
        for p in range(PIECES):
            tile_copies.append((
                quarter * quarter_cols < part_blocks * block,
                pltpu.make_async_copy(
                    part_refs[i * PIECES + p],
                    tiles.at[pl.ds(p * depth, depth), pl.ds(at, quarter_cols)],
                    part_sems.at[i * PIECES + p],
                ),
            ))
    for copy in query_copies + [key_copy]:
        copy.start()
    for used, copy in tile_copies:
        pl.when(used)(copy.start)
    value_copy.start()

    across = lax.broadcasted_iota(jnp.int32, (rows, rows), 1)
    down = lax.broadcasted_iota(jnp.int32, (rows, rows), 0)
    off = jnp.broadcast_to(off_ref[...], (rows, rows))
    off_down = jnp.max(jnp.where(across == down, off, 0), axis=1, keepdims=True)
    rank = jnp.sum(
        jnp.where((off_down < off) | ((off_down == off) & (down < across)), 1.0, 0.0), axis=0, keepdims=True
    ).astype(jnp.int32)
    rank_down = jnp.max(jnp.where(across == down, rank, 0), axis=1, keepdims=True)
    token = pltpu.roll(
        jnp.broadcast_to(tok_ref[...], (8, rows)), lax.rem(rows - member * local_rows, rows), axis=1
    )[:1]
    row_rank = jnp.max(jnp.where(down == token, rank_down, 0), axis=0, keepdims=True)
    order = (row_rank == down).astype(jnp.bfloat16)
    limit = jnp.max(jnp.where(rank == down, off, 0), axis=1, keepdims=True)
    wanted = lax.rem(member - down // local_rows + members, members) * local_rows + lax.rem(down, local_rows)
    leave = (jnp.max(jnp.where(across == wanted, rank, 0), axis=1, keepdims=True) == across).astype(jnp.bfloat16)

    before = lambda who: lax.fori_loop(0, who, lambda i, total: total + counts_ref[i], jnp.int32(0))
    own_base, part_base = before(member) * PAGE, before(partner) * PAGE

    def in_reach(g):
        last = jnp.max(limit[g * half:(g + 1) * half])
        own = jnp.clip((last - own_base + block - 1) // block, 0, own_blocks)
        return own, own + jnp.clip((last - part_base + block - 1) // block, 0, part_blocks)

    reach = [in_reach(g) for g in range(HALVES)]

    def place(g, b):
        own, _ = reach[g]
        return pl.multiple_of(jnp.where(b < own, b * block, cols + (b - own) * block), 128)

    spot = lax.broadcasted_iota(jnp.int32, (1, block), 1)

    def fill_bias(b, carry):
        at = place(HALVES - 1, b)
        own = at < cols
        inside = jnp.where(own, at, at - cols) + spot
        live = jnp.where(own, own_live, part_live) * PAGE
        positions = jnp.where(inside < live, jnp.where(own, own_base, part_base) + inside, FAR)
        bias[:, pl.ds(at, block)] = jnp.where(positions < limit, 0.0, FLOOR)
        return carry

    lax.fori_loop(0, reach[-1][1], fill_bias, 0)
    for copy in query_copies:
        copy.wait()
    turned[...] = jnp.dot(order, raw[...], preferred_element_type=jnp.float32).astype(jnp.bfloat16)
    key_copy.wait()
    for h in range(hh):
        lat = jnp.dot(turned[:, h * nope:(h + 1) * nope], wk[h], preferred_element_type=jnp.float32)
        lat = lat.astype(jnp.bfloat16)
        at = hh * nope + h * rope
        for g in range(HALVES):
            to = slice(g * group_rows + h * half, g * group_rows + (h + 1) * half)
            qs[to, :latent] = lat[g * half:(g + 1) * half]
            qs[to, latent:] = turned[g * half:(g + 1) * half, at:at + rope]
    mx[...] = jnp.full(mx.shape, FLOOR, jnp.float32)
    for used, copy in tile_copies:
        pl.when(used)(copy.wait)

    def score(g, b):
        at = place(g, b)
        scores = jnp.dot(
            qs[g * group_rows:(g + 1) * group_rows], tiles[:, pl.ds(at, block)], preferred_element_type=jnp.float32
        )
        shut = bias[g * half:(g + 1) * half, pl.ds(at, block)]
        for h in range(hh):
            part = slice(h * half, (h + 1) * half)
            value = scores[part] + shut
            sbuf[g, part, pl.ds(pl.multiple_of(b * block, 128), block)] = value
            top = functools.reduce(jnp.maximum, [value[:, i:i + 128] for i in range(0, block, 128)])
            mx[g, part] = jnp.maximum(mx[g, part], top)

    def gather(g, b, top):
        weights = jnp.exp2((sbuf[g, :, pl.ds(pl.multiple_of(b * block, 128), block)] - top) * scale2)
        den[...] += functools.reduce(jnp.add, [weights[:, i:i + 128] for i in range(0, block, 128)])
        acc[...] += lax.dot_general(
            weights.astype(jnp.bfloat16),
            tiles[:latent, pl.ds(place(g, b), block)],
            (((1,), (1,)), ((), ())),
            preferred_element_type=jnp.float32,
        )

    stats = []

    def close(g, top):
        total = jnp.sum(den[...], axis=1, keepdims=True)
        seen = top > 0.5 * FLOOR
        total = jnp.where(seen, total, 1.0)
        stats.append((jnp.where(seen, 1.0 / total, 0.0), jnp.where(seen, top * scale2 + jnp.log2(total), FLOOR)))
        for h in range(hh):
            sums[h, g * half:(g + 1) * half] = acc[h * half:(h + 1) * half].astype(jnp.bfloat16)

    def each(low, high, *steps):
        def body(b, carry):
            for step in steps:
                step(b)
            return carry

        lax.fori_loop(low, high, body, 0)

    each(0, reach[0][1], lambda b: score(0, b))
    for g in range(HALVES):
        top = jnp.max(mx[g], axis=1, keepdims=True)
        den[...] = jnp.zeros_like(den)
        acc[...] = jnp.zeros_like(acc)
        if g + 1 < HALVES:
            each(0, reach[g][1], lambda b: score(g + 1, b), lambda b: gather(g, b, top))
            each(reach[g][1], reach[g + 1][1], lambda b: score(g + 1, b))
        else:
            each(0, reach[g][1], lambda b: gather(g, b, top))
        close(g, top)

    value_copy.wait()
    lane = lax.broadcasted_iota(jnp.int32, (rows, 128), 1)
    logs = jnp.zeros((rows, 128), jnp.float32)
    for h in range(hh):
        part = slice(h * half, (h + 1) * half)
        value = jnp.dot(sums[h], wv[h], preferred_element_type=jnp.float32)
        value = value * jnp.concatenate([share[part] for share, _ in stats], axis=0)
        flat[:, h * vhead:(h + 1) * vhead] = value.astype(jnp.bfloat16)
        full = jnp.concatenate([log[part] for _, log in stats], axis=0)
        high = full.astype(jnp.bfloat16).astype(jnp.float32)
        middle = (full - high).astype(jnp.bfloat16).astype(jnp.float32)
        low = full - high - middle
        logs = jnp.where(lane == h, high, jnp.where(lane == hh + h, middle, jnp.where(lane == 2 * hh + h, low, logs)))
    flat[:, hh * vhead:] = logs.astype(jnp.bfloat16)
    ordered = jnp.dot(leave, flat[...], preferred_element_type=jnp.float32).astype(jnp.bfloat16)
    for s in range(members):
        out_refs[s][...] = ordered[s * local_rows:(s + 1) * local_rows]


def attend_call(members, hh, nope, rope, latent, vhead, rows, slots):
    hbm = pl.BlockSpec(memory_space=pltpu.HBM)
    vmem = pl.BlockSpec(memory_space=pltpu.VMEM)
    bf16, f32 = jnp.bfloat16, jnp.float32
    full = latent + rope
    cols = slots * PAGE
    local_rows = rows // members
    packed = hh * vhead + 128
    block = BLOCK_PAGES * PAGE
    own_blocks = -(-cols // block)
    group_rows = hh * (rows // HALVES)
    return pl.pallas_call(
        functools.partial(attend_kernel, (members, hh, nope, rope, latent, vhead, rows, slots)),
        out_shape=[jax.ShapeDtypeStruct((local_rows, packed), bf16)] * members,
        in_specs=[pl.BlockSpec(memory_space=pltpu.SMEM), vmem, vmem] + [hbm] * (members + LANES * PIECES + 3),
        out_specs=[vmem] * members,
        scratch_shapes=[
            pltpu.VMEM((rows, hh * (nope + rope)), bf16),
            pltpu.VMEM((rows, hh * (nope + rope)), bf16),
            pltpu.VMEM((hh, nope, latent), bf16),
            pltpu.VMEM((hh, latent, vhead), bf16),
            pltpu.VMEM((full, 2 * cols), bf16),
            pltpu.VMEM((rows, 2 * cols), f32),
            pltpu.VMEM((HALVES * group_rows, full), bf16),
            pltpu.VMEM((HALVES, group_rows, 2 * own_blocks * block), f32),
            pltpu.VMEM((HALVES, group_rows, 128), f32),
            pltpu.VMEM((group_rows, 128), f32),
            pltpu.VMEM((group_rows, latent), f32),
            pltpu.VMEM((hh, rows, latent), bf16),
            pltpu.VMEM((rows, packed), bf16),
            pltpu.SemaphoreType.DMA((2 + members,)),
            pltpu.SemaphoreType.DMA((own_blocks,)),
            pltpu.SemaphoreType.DMA((LANES * PIECES,)),
        ],
        compiler_params=pltpu.CompilerParams(vmem_limit_bytes=58 << 20),
        cost_estimate=pl.CostEstimate(flops=8 * 10**9, bytes_accessed=8 * 10**6, transcendentals=0),
        name="attend",
    )


def merge_kernel(dims, *refs):
    hh, vhead, members = dims
    out_ref = refs[-1]
    mine = lax.axis_index("pages") % GROUP
    for parity in range(GROUP):
        parts = [refs[s] for s in range(members) if s % GROUP == parity]
        logs = []
        for b in parts:
            packed = b[:, hh * vhead:].astype(jnp.float32)
            logs.append(packed[:, :hh] + packed[:, hh:2 * hh] + packed[:, 2 * hh:3 * hh])
        top = functools.reduce(jnp.maximum, logs)
        weights = [jnp.exp2(v - top) for v in logs]
        total = functools.reduce(jnp.add, weights)
        weights = [w / total for w in weights]
        base = lax.rem(mine + parity, GROUP) * (hh * vhead)
        for h in range(hh):
            cols = slice(h * vhead, (h + 1) * vhead)
            value = functools.reduce(
                jnp.add, [w[:, h:h + 1] * b[:, cols].astype(jnp.float32) for w, b in zip(weights, parts)]
            )
            out_ref[:, pl.ds(pl.multiple_of(base + h * vhead, 128), vhead)] = value.astype(jnp.bfloat16)


def on_device(
    q_nope, q_rope, cache_tiles, absorb_keys, absorb_values, page_counts, query_token, query_offsets, members, devices
):
    heads_here, nope, latent = absorb_keys.shape
    vhead = absorb_values.shape[2]
    local_rows = q_nope.shape[0]
    rope = q_rope.shape[1] // heads_here
    full = cache_tiles.shape[1]
    slots = cache_tiles.shape[0] // PAGE
    cols = slots * PAGE
    rows = local_rows * members
    hh = heads_here // GROUP
    hbm = pl.BlockSpec(memory_space=pltpu.HBM)
    vmem = pl.BlockSpec(memory_space=pltpu.VMEM)
    bf16 = jnp.bfloat16

    def over_pages(x, s):
        return lax.ppermute(x, "pages", [(i, (i - s) % members) for i in range(members)])

    def over_heads(x, bit):
        return lax.ppermute(x, "heads", [(i, i ^ bit) for i in range(devices)])

    turned = cache_tiles.T
    pieces = pl.pallas_call(
        functools.partial(pack_pages_kernel, cols // LANES),
        out_shape=[jax.ShapeDtypeStruct((full // PIECES, cols // LANES), bf16)] * PIECES,
        in_specs=[hbm],
        out_specs=[vmem] * PIECES,
        scratch_shapes=[pltpu.SemaphoreType.DMA((PIECES,))],
        name="pack_pages",
    )(turned)
    shares = pl.pallas_call(
        functools.partial(pack_queries_kernel, (hh * nope, hh * rope)),
        out_shape=[jax.ShapeDtypeStruct((local_rows, hh * (nope + rope)), bf16)] * GROUP,
        in_specs=[hbm] * 2,
        out_specs=[vmem] * GROUP,
        scratch_shapes=[pltpu.SemaphoreType.DMA((2 * GROUP,))],
        name="pack_queries",
    )(q_nope, q_rope)

    parts = [[None] * PIECES for _ in range(LANES)]
    for p in range(PIECES):
        parts[0][p] = lax.ppermute(pieces[p], "pages", [(i, i ^ 1) for i in range(members)])
        parts[1][p] = over_heads(parts[0][p], 2)
        parts[2][p] = over_heads(parts[0][p], 1)
        parts[3][p] = over_heads(parts[1][p], 1)
    parts = [p for part in parts for p in part]
    queries = [shares[0]]
    for s in range(1, members):
        queries.append(over_pages(shares[s % GROUP], s))
    outs = attend_call(members, hh, nope, rope, latent, vhead, rows, slots)(
        page_counts, query_token[None, :], query_offsets[None, :], *queries, *parts, turned, absorb_keys, absorb_values
    )
    arrived = [outs[0]]
    for s in range(1, members):
        arrived.append(over_pages(outs[s], s))

    return pl.pallas_call(
        functools.partial(merge_kernel, (hh, vhead, members)),
        out_shape=jax.ShapeDtypeStruct((local_rows, heads_here * vhead), bf16),
        in_specs=[vmem] * members,
        out_specs=vmem,
        name="merge",
    )(*arrived)


def solution(mesh):
    in_specs = (
        P(("groups", "pages"), "heads"),
        P(("groups", "pages"), "heads"),
        P(("groups", "pages"), None),
        P("heads", None, None),
        P("heads", None, None),
        P("groups"),
        P("groups"),
        P("groups"),
    )
    body = functools.partial(on_device, members=mesh.shape["pages"], devices=mesh.shape["heads"])
    return jax.shard_map(
        body, mesh=mesh, in_specs=in_specs, out_specs=P(("groups", "pages"), "heads"), check_vma=False
    )
```

```python
import functools

import jax
import jax.numpy as jnp
from jax import lax
from jax.experimental import pallas as pl
from jax.experimental.pallas import tpu as pltpu
from jax.sharding import PartitionSpec as P


PAGE = 64
GROUP = 2
LANES = 4
BLOCK_PAGES = 8
PIECES = 2
HALVES = 2


FLOOR = -1e30
FAR = 2**30
LOG2E = 1.4426950408889634


def pack_pages_kernel(quarter_cols, cache_ref, *refs):
    outs, sems = refs[:-1], refs[-1]
    lane = lax.axis_index("heads") % LANES
    depth = cache_ref.shape[0] // PIECES
    at = pl.ds(pl.multiple_of(lane * quarter_cols, 128), quarter_cols)
    copies = [
        pltpu.make_async_copy(cache_ref.at[pl.ds(p * depth, depth), at], outs[p], sems.at[p]) for p in range(PIECES)
    ]
    for c in copies:
        c.start()
    for c in copies:
        c.wait()


def pack_queries_kernel(dims, nope_ref, rope_ref, *refs):
    nope_width, rope_width = dims
    outs, sems = refs[:-1], refs[-1]
    mine = lax.axis_index("pages") % GROUP
    copies = []
    for e in range(GROUP):
        which = (mine + e) % GROUP
        for ref, width, at in ((nope_ref, nope_width, 0), (rope_ref, rope_width, nope_width)):
            copies.append(
                pltpu.make_async_copy(
                    ref.at[:, pl.ds(pl.multiple_of(which * width, 128), width)],
                    outs[e].at[:, pl.ds(at, width)],
                    sems.at[len(copies)],
                )
            )
    for c in copies:
        c.start()
    for c in copies:
        c.wait()


def attend_kernel(dims, counts_ref, tok_ref, off_ref, *refs):
    members, hh, nope, rope, latent, vhead, rows, slots = dims
    q_refs, refs = refs[:members], refs[members:]
    part_refs, refs = refs[:LANES * PIECES], refs[LANES * PIECES:]
    own_ref, keys_hbm, values_hbm = refs[:3]
    out_refs, refs = refs[3:3 + members], refs[3 + members:]
    turned, wk, wv, tiles, bias, qs, sbuf, mx, den, acc, sums, flat, sems, own_sems = refs
    local_rows = rows // members
    block = BLOCK_PAGES * PAGE
    cols = slots * PAGE
    quarter_cols = cols // LANES
    depth = (latent + rope) // PIECES
    scale2 = (nope + rope) ** (-0.5) * LOG2E
    half = rows // HALVES
    group_rows = hh * half
    member = lax.axis_index("pages")
    lane_id = lax.axis_index("heads") % LANES
    partner = member ^ 1
    mine = member % GROUP
    own_live, part_live = counts_ref[member], counts_ref[partner]
    own_blocks = (own_live + BLOCK_PAGES - 1) // BLOCK_PAGES
    part_blocks = (part_live + BLOCK_PAGES - 1) // BLOCK_PAGES

    tile_copies = []
    for b in range(-(-cols // block)):
        at = pl.ds(b * block, min(block, cols - b * block))
        tile_copies.append((b < own_blocks, pltpu.make_async_copy(own_ref.at[:, at], tiles.at[:, at], own_sems.at[b])))
    key_copy = pltpu.make_async_copy(keys_hbm.at[pl.ds(mine * hh, hh)], wk, sems.at[0])
    value_copy = pltpu.make_async_copy(values_hbm.at[pl.ds(mine * hh, hh)], wv, sems.at[1])
    key_copy.start()
    for used, copy in tile_copies:
        pl.when(used)(copy.start)
    for i, flip in enumerate((0, 2, 1, 3)):
        quarter = lane_id ^ flip
        at = pl.multiple_of(cols + quarter * quarter_cols, 128)

        @pl.when(quarter * quarter_cols < part_blocks * block)
        def _(i=i, at=at):
            for p in range(PIECES):
                tiles[p * depth:(p + 1) * depth, pl.ds(at, quarter_cols)] = part_refs[i * PIECES + p][...]

    mx[...] = jnp.full(mx.shape, FLOOR, jnp.float32)
    den[...] = jnp.zeros_like(den)
    acc[...] = jnp.zeros_like(acc)

    across = lax.broadcasted_iota(jnp.int32, (rows, rows), 1)
    down = lax.broadcasted_iota(jnp.int32, (rows, rows), 0)
    off = jnp.broadcast_to(off_ref[...], (rows, rows))
    off_down = jnp.max(jnp.where(across == down, off, 0), axis=1, keepdims=True)
    rank = jnp.sum(
        jnp.where((off_down < off) | ((off_down == off) & (down < across)), 1.0, 0.0), axis=0, keepdims=True
    ).astype(jnp.int32)
    rank_down = jnp.max(jnp.where(across == down, rank, 0), axis=1, keepdims=True)
    token = pltpu.roll(
        jnp.broadcast_to(tok_ref[...], (8, rows)), lax.rem(rows - member * local_rows, rows), axis=1
    )[:1]
    row_rank = jnp.max(jnp.where(down == token, rank_down, 0), axis=0, keepdims=True)
    order = (row_rank == down).astype(jnp.bfloat16)
    limit = jnp.max(jnp.where(rank == down, off, 0), axis=1, keepdims=True)
    wanted = lax.rem(member - down // local_rows + members, members) * local_rows + lax.rem(down, local_rows)
    leave = (jnp.max(jnp.where(across == wanted, rank, 0), axis=1, keepdims=True) == across).astype(jnp.bfloat16)

    before = lambda who: lax.fori_loop(0, who, lambda i, total: total + counts_ref[i], jnp.int32(0))
    own_base, part_base = before(member) * PAGE, before(partner) * PAGE

    def in_reach(g):
        last = jnp.max(limit[g * half:(g + 1) * half])
        own = jnp.clip((last - own_base + block - 1) // block, 0, own_blocks)
        return own, own + jnp.clip((last - part_base + block - 1) // block, 0, part_blocks)

    reach = [in_reach(g) for g in range(HALVES)]

    def place(g, b):
        own, _ = reach[g]
        return pl.multiple_of(jnp.where(b < own, b * block, cols + (b - own) * block), 128)

    spot = lax.broadcasted_iota(jnp.int32, (1, block), 1)

    def fill_bias(b, carry):
        at = place(HALVES - 1, b)
        own = at < cols
        inside = jnp.where(own, at, at - cols) + spot
        live = jnp.where(own, own_live, part_live) * PAGE
        positions = jnp.where(inside < live, jnp.where(own, own_base, part_base) + inside, FAR)
        bias[:, pl.ds(at, block)] = jnp.where(positions < limit, 0.0, FLOOR)
        return carry

    lax.fori_loop(0, reach[-1][1], fill_bias, 0)
    whole = jnp.concatenate([q[...] for q in q_refs], axis=0)
    turned[...] = jnp.dot(order, whole, preferred_element_type=jnp.float32).astype(jnp.bfloat16)
    key_copy.wait()
    for h in range(hh):
        lat = jnp.dot(turned[:, h * nope:(h + 1) * nope], wk[h], preferred_element_type=jnp.float32)
        lat = lat.astype(jnp.bfloat16)
        at = hh * nope + h * rope
        for g in range(HALVES):
            to = slice(g * group_rows + h * half, g * group_rows + (h + 1) * half)
            qs[to, :latent] = lat[g * half:(g + 1) * half]
            qs[to, latent:] = turned[g * half:(g + 1) * half, at:at + rope]
    value_copy.start()
    for used, copy in tile_copies:
        pl.when(used)(copy.wait)

    def score(g, b):
        at = place(g, b)
        scores = jnp.dot(
            qs[g * group_rows:(g + 1) * group_rows], tiles[:, pl.ds(at, block)], preferred_element_type=jnp.float32
        )
        shut = bias[g * half:(g + 1) * half, pl.ds(at, block)]
        for h in range(hh):
            part = slice(h * half, (h + 1) * half)
            value = scores[part] + shut
            sbuf[part, pl.ds(pl.multiple_of(b * block, 128), block)] = value
            top = functools.reduce(jnp.maximum, [value[:, i:i + 128] for i in range(0, block, 128)])
            mx[g, part] = jnp.maximum(mx[g, part], top)

    def gather(g, b, top):
        weights = jnp.exp2((sbuf[:, pl.ds(pl.multiple_of(b * block, 128), block)] - top) * scale2)
        den[g] += functools.reduce(jnp.add, [weights[:, i:i + 128] for i in range(0, block, 128)])
        acc[g] += lax.dot_general(
            weights.astype(jnp.bfloat16),
            tiles[:latent, pl.ds(place(g, b), block)],
            (((1,), (1,)), ((), ())),
            preferred_element_type=jnp.float32,
        )

    stats = []

    def close(g, top):
        total = jnp.sum(den[g], axis=1, keepdims=True)
        seen = top > 0.5 * FLOOR
        total = jnp.where(seen, total, 1.0)
        stats.append((jnp.where(seen, 1.0 / total, 0.0), jnp.where(seen, top * scale2 + jnp.log2(total), FLOOR)))
        for h in range(hh):
            sums[h, g * half:(g + 1) * half] = acc[g, h * half:(h + 1) * half].astype(jnp.bfloat16)

    def each(low, high, *steps):
        def body(b, carry):
            for step in steps:
                step(b)
            return carry

        lax.fori_loop(low, high, body, 0)

    each(0, reach[0][1], lambda b: score(0, b))
    for g in range(HALVES):
        top = jnp.max(mx[g], axis=1, keepdims=True)
        if g + 1 < HALVES:
            each(0, reach[g][1], lambda b: gather(g, b, top), lambda b: score(g + 1, b))
            each(reach[g][1], reach[g + 1][1], lambda b: score(g + 1, b))
        else:
            each(0, reach[g][1], lambda b: gather(g, b, top))
        close(g, top)

    value_copy.wait()
    lane = lax.broadcasted_iota(jnp.int32, (rows, 128), 1)
    logs = jnp.zeros((rows, 128), jnp.float32)
    for h in range(hh):
        part = slice(h * half, (h + 1) * half)
        value = jnp.dot(sums[h], wv[h], preferred_element_type=jnp.float32)
        value = value * jnp.concatenate([share[part] for share, _ in stats], axis=0)
        flat[:, h * vhead:(h + 1) * vhead] = value.astype(jnp.bfloat16)
        full = jnp.concatenate([log[part] for _, log in stats], axis=0)
        high = full.astype(jnp.bfloat16).astype(jnp.float32)
        middle = (full - high).astype(jnp.bfloat16).astype(jnp.float32)
        low = full - high - middle
        logs = jnp.where(lane == h, high, jnp.where(lane == hh + h, middle, jnp.where(lane == 2 * hh + h, low, logs)))
    flat[:, hh * vhead:] = logs.astype(jnp.bfloat16)
    ordered = jnp.dot(leave, flat[...], preferred_element_type=jnp.float32).astype(jnp.bfloat16)
    for s in range(members):
        out_refs[s][...] = ordered[s * local_rows:(s + 1) * local_rows]


def attend_call(members, hh, nope, rope, latent, vhead, rows, slots):
    hbm = pl.BlockSpec(memory_space=pltpu.HBM)
    vmem = pl.BlockSpec(memory_space=pltpu.VMEM)
    bf16, f32 = jnp.bfloat16, jnp.float32
    full = latent + rope
    cols = slots * PAGE
    local_rows = rows // members
    packed = hh * vhead + 128
    block = BLOCK_PAGES * PAGE
    own_blocks = -(-cols // block)
    group_rows = hh * (rows // HALVES)
    return pl.pallas_call(
        functools.partial(attend_kernel, (members, hh, nope, rope, latent, vhead, rows, slots)),
        out_shape=[jax.ShapeDtypeStruct((local_rows, packed), bf16)] * members,
        in_specs=[pl.BlockSpec(memory_space=pltpu.SMEM)] + [vmem] * (2 + members + LANES * PIECES) + [hbm] * 3,
        out_specs=[vmem] * members,
        scratch_shapes=[
            pltpu.VMEM((rows, hh * (nope + rope)), bf16),
            pltpu.VMEM((hh, nope, latent), bf16),
            pltpu.VMEM((hh, latent, vhead), bf16),
            pltpu.VMEM((full, 2 * cols), bf16),
            pltpu.VMEM((rows, 2 * cols), f32),
            pltpu.VMEM((HALVES * group_rows, full), bf16),
            pltpu.VMEM((group_rows, 2 * own_blocks * block), f32),
            pltpu.VMEM((HALVES, group_rows, 128), f32),
            pltpu.VMEM((HALVES, group_rows, 128), f32),
            pltpu.VMEM((HALVES, group_rows, latent), f32),
            pltpu.VMEM((hh, rows, latent), bf16),
            pltpu.VMEM((rows, packed), bf16),
            pltpu.SemaphoreType.DMA((2,)),
            pltpu.SemaphoreType.DMA((own_blocks,)),
        ],
        compiler_params=pltpu.CompilerParams(vmem_limit_bytes=48 << 20),
        cost_estimate=pl.CostEstimate(flops=8 * 10**9, bytes_accessed=8 * 10**6, transcendentals=0),
        name="attend",
    )


def merge_kernel(dims, *refs):
    hh, vhead, members = dims
    out_ref = refs[-1]
    mine = lax.axis_index("pages") % GROUP
    for parity in range(GROUP):
        parts = [refs[s] for s in range(members) if s % GROUP == parity]
        logs = []
        for b in parts:
            packed = b[:, hh * vhead:].astype(jnp.float32)
            logs.append(packed[:, :hh] + packed[:, hh:2 * hh] + packed[:, 2 * hh:3 * hh])
        top = functools.reduce(jnp.maximum, logs)
        weights = [jnp.exp2(v - top) for v in logs]
        total = functools.reduce(jnp.add, weights)
        weights = [w / total for w in weights]
        base = lax.rem(mine + parity, GROUP) * (hh * vhead)
        for h in range(hh):
            cols = slice(h * vhead, (h + 1) * vhead)
            value = functools.reduce(
                jnp.add, [w[:, h:h + 1] * b[:, cols].astype(jnp.float32) for w, b in zip(weights, parts)]
            )
            out_ref[:, pl.ds(pl.multiple_of(base + h * vhead, 128), vhead)] = value.astype(jnp.bfloat16)


def on_device(
    q_nope, q_rope, cache_tiles, absorb_keys, absorb_values, page_counts, query_token, query_offsets, members, devices
):
    heads_here, nope, latent = absorb_keys.shape
    vhead = absorb_values.shape[2]
    local_rows = q_nope.shape[0]
    rope = q_rope.shape[1] // heads_here
    full = cache_tiles.shape[1]
    slots = cache_tiles.shape[0] // PAGE
    cols = slots * PAGE
    rows = local_rows * members
    hh = heads_here // GROUP
    hbm = pl.BlockSpec(memory_space=pltpu.HBM)
    vmem = pl.BlockSpec(memory_space=pltpu.VMEM)
    bf16 = jnp.bfloat16

    def over_pages(x, s):
        return lax.ppermute(x, "pages", [(i, (i - s) % members) for i in range(members)])

    def over_heads(x, bit):
        return lax.ppermute(x, "heads", [(i, i ^ bit) for i in range(devices)])

    turned = cache_tiles.T
    pieces = pl.pallas_call(
        functools.partial(pack_pages_kernel, cols // LANES),
        out_shape=[jax.ShapeDtypeStruct((full // PIECES, cols // LANES), bf16)] * PIECES,
        in_specs=[hbm],
        out_specs=[vmem] * PIECES,
        scratch_shapes=[pltpu.SemaphoreType.DMA((PIECES,))],
        compiler_params=pltpu.CompilerParams(vmem_limit_bytes=8 << 20),
        name="pack_pages",
    )(turned)
    shares = pl.pallas_call(
        functools.partial(pack_queries_kernel, (hh * nope, hh * rope)),
        out_shape=[jax.ShapeDtypeStruct((local_rows, hh * (nope + rope)), bf16)] * GROUP,
        in_specs=[hbm] * 2,
        out_specs=[vmem] * GROUP,
        scratch_shapes=[pltpu.SemaphoreType.DMA((2 * GROUP,))],
        cost_estimate=pl.CostEstimate(flops=3 * 10**10, bytes_accessed=10**6, transcendentals=0),
        compiler_params=pltpu.CompilerParams(vmem_limit_bytes=8 << 20),
        name="pack_queries",
    )(q_nope, q_rope)

    parts = [[None] * PIECES for _ in range(LANES)]
    for p in range(PIECES):
        parts[0][p] = lax.ppermute(pieces[p], "pages", [(i, i ^ 1) for i in range(members)])
        parts[1][p] = over_heads(parts[0][p], 2)
        parts[2][p] = over_heads(parts[0][p], 1)
        parts[3][p] = over_heads(parts[1][p], 1)
    parts = [p for part in parts for p in part]
    queries = [shares[0]]
    for s in range(1, members):
        queries.append(over_pages(shares[s % GROUP], s))
    outs = attend_call(members, hh, nope, rope, latent, vhead, rows, slots)(
        page_counts, query_token[None, :], query_offsets[None, :], *queries, *parts, turned, absorb_keys, absorb_values
    )
    arrived = [outs[0]]
    for s in range(1, members):
        arrived.append(over_pages(outs[s], s))

    return pl.pallas_call(
        functools.partial(merge_kernel, (hh, vhead, members)),
        out_shape=jax.ShapeDtypeStruct((local_rows, heads_here * vhead), bf16),
        in_specs=[vmem] * members,
        out_specs=vmem,
        compiler_params=pltpu.CompilerParams(vmem_limit_bytes=16 << 20),
        name="merge",
    )(*arrived)


def solution(mesh):
    in_specs = (
        P(("groups", "pages"), "heads"),
        P(("groups", "pages"), "heads"),
        P(("groups", "pages"), None),
        P("heads", None, None),
        P("heads", None, None),
        P("groups"),
        P("groups"),
        P("groups"),
    )
    body = functools.partial(on_device, members=mesh.shape["pages"], devices=mesh.shape["heads"])
    return jax.shard_map(
        body, mesh=mesh, in_specs=in_specs, out_specs=P(("groups", "pages"), "heads"), check_vma=False
    )
```
